128 devices in a mesh: dp: 1, tpa: 2 (over core), tpb: 64 (over z, y, x).
Axes of the slice: x: 4, y: 4, z: 4, core: 2. Of those that a mesh axis runs over, the one named last changes fastest.
Arguments:
- hidden: bfloat16 [1024, 5, 4096], P('dp')
- w_head: bfloat16 [4096, 32768], P(None, ('tpa', 'tpb'))
- q_draft: float32 [1024, 4, 32768], P(('dp', 'tpa', 'tpb'))
- x_draft: int32 [1024, 4], P('dp')
Outputs:
- output 1: float32 [1024, 4], P('dp')
- output 2: float32 [1024], P('dp')
- output 3: float32 [1024, 4, 32768], P('dp', None, ('tpa', 'tpb'))
- output 4: float32 [1024, 32768], P('dp', ('tpa', 'tpb'))
All inputs are finite; a program needn't handle non-finite values.
Results may differ from the reference program's by a relative error of at most 0.001.
Values are sent between devices in bfloat16 or wider.
A program may use at most 1 GiB of HBM per device.

```python
import jax
import jax.numpy as jnp
from jax import lax

NUM_SEQS = 1024
NUM_DRAFT = 4
D_MODEL = 4096
VOCAB_SIZE = 32768
ROW_BLOCK = 8
INV_TEMP = 1.25
DRAFT_LOGIT_SCALE = 0.5


def draw_tokens(tok_key):
    key_vals, key_low, key_high = jax.random.split(tok_key, 3)
    n_total = NUM_SEQS * NUM_DRAFT
    tokens = jax.random.randint(key_vals, (n_total,), 0, VOCAB_SIZE, jnp.int32)
    low_slot = jax.random.randint(key_low, (), 0, n_total, jnp.int32)
    high_slot = (low_slot + 1 + jax.random.randint(key_high, (), 0, n_total - 1, jnp.int32)) % n_total
    slots = jnp.arange(n_total, dtype=jnp.int32)
    tokens = jnp.where(slots == low_slot, 0, tokens)
    tokens = jnp.where(slots == high_slot, VOCAB_SIZE - 1, tokens)
    return tokens.reshape(NUM_SEQS, NUM_DRAFT)


def setup_inputs(seed: int = 0, part: int = 0) -> dict:
    base_key = jax.random.key(seed)
    part_key = jax.random.fold_in(base_key, part)
    key_hidden, key_draft, key_tok = jax.random.split(part_key, 3)
    hidden = jax.random.normal(key_hidden, (NUM_SEQS, NUM_DRAFT + 1, D_MODEL), jnp.float32)
    w_head = jax.random.normal(jax.random.key(seed + 1), (D_MODEL, VOCAB_SIZE), jnp.float32) * D_MODEL ** -0.5
    draft_logits = jax.random.normal(key_draft, (NUM_SEQS, NUM_DRAFT, VOCAB_SIZE), jnp.float32) * DRAFT_LOGIT_SCALE
    q_draft = jax.nn.softmax(draft_logits, axis=-1)
    x_draft = draw_tokens(key_tok)
    return {"hidden": hidden.astype(jnp.bfloat16), "w_head": w_head.astype(jnp.bfloat16), "q_draft": q_draft, "x_draft": x_draft}


def reference(hidden, w_head, q_draft, x_draft):
    num_blocks = NUM_SEQS // ROW_BLOCK

    def one_block(block):
        hid_blk, q_blk, tok_blk = block
        flat_hid = hid_blk.reshape(ROW_BLOCK * (NUM_DRAFT + 1), D_MODEL)
        logits = jnp.dot(flat_hid, w_head, preferred_element_type=jnp.float32) * INV_TEMP
        prob_all = jax.nn.softmax(logits, axis=-1).reshape(ROW_BLOCK, NUM_DRAFT + 1, VOCAB_SIZE)
        p_draft = prob_all[:, :NUM_DRAFT, :]
        tok_idx = tok_blk[:, :, None]
        p_pick = jnp.take_along_axis(p_draft, tok_idx, axis=2)[:, :, 0]
        q_pick = jnp.take_along_axis(q_blk, tok_idx, axis=2)[:, :, 0]
        accept = jnp.minimum(1.0, p_pick / q_pick)
        excess = jnp.maximum(p_draft - q_blk, 0.0)
        residual = excess / jnp.sum(excess, axis=-1, keepdims=True)
        return accept, residual, prob_all[:, NUM_DRAFT, :]

    block_outs = lax.map(one_block, (
        hidden.reshape(num_blocks, ROW_BLOCK, NUM_DRAFT + 1, D_MODEL),
        q_draft.reshape(num_blocks, ROW_BLOCK, NUM_DRAFT, VOCAB_SIZE),
        x_draft.reshape(num_blocks, ROW_BLOCK, NUM_DRAFT)))
    accept = block_outs[0].reshape(NUM_SEQS, NUM_DRAFT)
    residual = block_outs[1].reshape(NUM_SEQS, NUM_DRAFT, VOCAB_SIZE)
    bonus_prob = block_outs[2].reshape(NUM_SEQS, VOCAB_SIZE)
    expected = jnp.sum(jnp.cumprod(accept, axis=1), axis=1)
    return accept, expected, residual, bonus_prob
```

```python
import functools

import jax
import jax.numpy as jnp
from jax import lax
from jax.experimental import pallas as pl
from jax.experimental.pallas import tpu as pltpu
from jax.sharding import PartitionSpec as P

INV_TEMP = 1.25
VOCAB_AXES = ("tpa", "tpb")
MESH = pl.DeviceIdType.MESH
F32 = jnp.float32
LANES = 128
CHUNKS = ((0, 4), (4, 1), (5, 2), (7, 1))
ROWS = 256
NBUF = 3


def kernel(dims, h_ref, w_ref, q_ref, x_ref, acc_ref, exp_ref, res_ref, bon_ref,
           hbuf, wbuf, qsrc, qdst, zr, z4, zb, st_send, st_recv, ag_send, ag_recv, zs_send, zs_recv, za_send, za_recv,
           zb_recv, h_sem, w_sem, q_sem, out_sem, bulk_ss, bulk_rs, st_ss, st_rs, ag_ss, ag_rs, zs_ss, zs_rs, za_ss,
           za_rs, zc_ss, zc_rs):
    na, nb = dims
    nd = na * nb
    me_a, me_b = lax.axis_index("tpa"), lax.axis_index("tpb")
    me = me_a * nb + me_b
    npos = h_ref.shape[0]
    ndraft = npos - 1
    nseq = h_ref.shape[1]
    nblk = nseq // LANES
    nunit = nblk * npos
    per_src = nseq // nd
    vloc = w_ref.shape[1]

    def dev(f):
        return {"tpa": f // nb, "tpb": f % nb}

    def peer(k):
        ka, kb = k % na, k // na
        kx, ky, kz = kb % 4, (kb // 4) % 4, kb // 16
        x, y, z = me_b % 4, (me_b // 4) % 4, me_b // 16
        b = ((z + kz) % 4) * 16 + ((y + ky) % 4) * 4 + (x + kx) % 4
        return ((me_a + ka) % na) * nb + b

    def each_peer(fn):
        def body(k, carry):
            fn(peer(k))
            return carry
        lax.fori_loop(1, nd, body, 0)

    lane = lax.broadcasted_iota(jnp.int32, (8, LANES), 1)
    sub = lax.broadcasted_iota(jnp.int32, (8, LANES), 0)
    sub4 = lax.broadcasted_iota(jnp.int32, (4, LANES), 0)
    lane_f = lane.astype(F32)
    eye = (lax.broadcasted_iota(jnp.int32, (LANES, LANES), 0) == lax.broadcasted_iota(jnp.int32, (LANES, LANES), 1))

    def to_col(row):
        return jnp.sum(jnp.where(eye, jnp.broadcast_to(row, (LANES, LANES)), 0.0), axis=1, keepdims=True)

    def to_row(col):
        return jnp.sum(jnp.where(eye, jnp.broadcast_to(col, (LANES, LANES)), 0.0), axis=0, keepdims=True)

    def twice(t):
        return jnp.concatenate([t, t], axis=0)

    q_copy = pltpu.make_async_copy(q_ref, qsrc, q_sem)
    q_copy.start()
    w_copy = pltpu.make_async_copy(w_ref, wbuf, w_sem)
    w_copy.start()
    per_pos = nseq // ROWS

    def h_copy(t):
        return pltpu.make_async_copy(h_ref.at[t // per_pos, pl.ds((t % per_pos) * ROWS, ROWS)], hbuf.at[t % NBUF],
                                     h_sem.at[t % NBUF])

    for t in range(NBUF - 1):
        h_copy(t).start()

    barrier = pltpu.get_barrier_semaphore()
    each_peer(lambda f: pl.semaphore_signal(barrier, inc=1, device_id=dev(f), device_id_type=MESH))
    q_copy.wait()

    def local_bulk(g):
        c0, n = CHUNKS[g]
        return pltpu.make_async_copy(qsrc.at[pl.ds(c0, n), me], qdst.at[me, pl.ds(c0, n)], bulk_rs.at[g])

    for g in range(len(CHUNKS)):
        local_bulk(g).start()
    pl.semaphore_wait(barrier, nd - 1)

    def send_bulk(g):
        c0, n = CHUNKS[g]
        each_peer(lambda f: pltpu.make_async_remote_copy(
            src_ref=qsrc.at[pl.ds(c0, n), f], dst_ref=qdst.at[me, pl.ds(c0, n)], send_sem=bulk_ss.at[g],
            recv_sem=bulk_rs.at[g], device_id=dev(f), device_id_type=MESH).start())

    def wait_bulk(g):
        c0, n = CHUNKS[g]
        ref = qdst.at[:, pl.ds(c0, n)]
        pltpu.make_async_copy(ref, ref, bulk_rs.at[g]).wait()

    send_bulk(0)

    xb = x_ref[:, pl.ds(pl.multiple_of((me // 16) * LANES, LANES), LANES)].astype(F32)
    targets = []
    for c in range(per_src):
        j = (me % 16) * per_src + c
        col = jnp.sum(jnp.where(lane[:4] == j, xb, 0.0), axis=1, keepdims=True)
        targets.append(twice(jnp.broadcast_to(col, (4, LANES))) - jnp.where(sub >= 4, F32(LANES), F32(0)) - lane_f)

    def pick_q(d, accs):
        base = (d * vloc).astype(F32)
        return tuple(a + jnp.where(t == base, qsrc[c, d], 0.0) for c, (a, t) in enumerate(zip(accs, targets)))

    accs = lax.fori_loop(0, nd, pick_q, tuple(jnp.zeros((8, LANES), F32) for _ in range(per_src)))
    qp = jnp.zeros((4, LANES), F32)
    for c in range(per_src):
        col = jnp.sum(accs[c], axis=1, keepdims=True)
        qp = jnp.where(lane[:4] == (me % 16) * per_src + c, col[:4] + col[4:], qp)

    w_copy.wait()
    my_base = (me * vloc).astype(F32)
    lane2 = lax.broadcasted_iota(jnp.int32, (LANES, vloc), 1).astype(F32)

    def matmul(t, carry):
        @pl.when(t + NBUF - 1 < npos * per_pos)
        def _():
            h_copy(t + NBUF - 1).start()

        h_copy(t).wait()
        i, r = t // per_pos, t % per_pos
        zb[...] = jnp.dot(hbuf[t % NBUF], wbuf[...], preferred_element_type=F32) * INV_TEMP
        for half in range(ROWS // LANES):
            blk = r * (ROWS // LANES) + half
            zz = zb[half * LANES:(half + 1) * LANES, :]
            m = jnp.max(zz, axis=1, keepdims=True)
            s = jnp.sum(jnp.exp(zz - m), axis=1, keepdims=True)
            ii = jnp.minimum(i, ndraft - 1)
            xblk = x_ref[:, pl.ds(pl.multiple_of(blk * LANES, LANES), LANES)].astype(F32)
            xrow = jnp.sum(jnp.where(sub4 == ii, xblk, 0.0), axis=0, keepdims=True) - my_base
            pick = jnp.sum(jnp.where(lane2 == to_col(xrow), zz, 0.0), axis=1, keepdims=True)
            qrow = jnp.sum(jnp.where((sub4 == ii) & (blk == me // 16), qp, 0.0), axis=0, keepdims=True)
            tile = jnp.where(sub4 == 0, to_row(m), jnp.where(sub4 == 1, to_row(s), jnp.where(
                sub4 == 2, to_row(pick), qrow)))
            st_send[blk * npos + i] = tile

            @pl.when(i < ndraft)
            def _():
                for lt in range(vloc // LANES):
                    zr[pl.ds(blk * LANES * 8 + lt * 4 + i, LANES, stride=8), :] = zz[:, lt * LANES:(lt + 1) * LANES]

            @pl.when(i == ndraft)
            def _():
                z4[pl.ds(pl.multiple_of(blk * LANES, LANES), LANES), :] = zz
        return carry

    lax.fori_loop(0, npos * per_pos, matmul, 0)

    def owner(u):
        return u * 3

    is_owner = (me % 3 == 0) & (me < nunit * 3)
    my_unit = me // 3

    def send_stats(u, carry):
        f = owner(u)

        @pl.when(f != me)
        def _():
            pltpu.make_async_remote_copy(src_ref=st_send.at[u], dst_ref=st_recv.at[me], send_sem=st_ss, recv_sem=st_rs,
                                         device_id=dev(f), device_id_type=MESH).start()
        return carry

    lax.fori_loop(0, nunit, send_stats, 0)
    send_bulk(1)

    @pl.when(is_owner)
    def _():
        pltpu.make_async_copy(st_send.at[my_unit], st_recv.at[me], st_rs).start()
        pltpu.make_async_copy(st_recv, st_recv, st_rs).wait()
        mx = lax.fori_loop(0, nd, lambda s, m: jnp.maximum(m, st_recv[s]), st_recv[0])[0:1]

        def add(s, carry):
            t = st_recv[s]
            es, zp, qq = carry
            return es + jnp.exp(t[0:1] - mx) * t[1:2], zp + t[2:3], qq + t[3:4]

        zero = jnp.zeros((1, LANES), F32)
        es, zp, qq = lax.fori_loop(0, nd, add, (zero, zero, zero))
        accept = jnp.minimum(1.0, jnp.exp(zp - mx) / es / qq)
        ag_send[...] = jnp.where(sub4 == 0, mx, jnp.where(sub4 == 1, 1.0 / es, accept))
        pltpu.make_async_copy(ag_send, ag_recv.at[my_unit], ag_rs).start()
        each_peer(lambda f: pltpu.make_async_remote_copy(
            src_ref=ag_send, dst_ref=ag_recv.at[my_unit], send_sem=ag_ss, recv_sem=ag_rs, device_id=dev(f),
            device_id_type=MESH).start())

    send_bulk(2)

    pltpu.make_async_copy(ag_recv, ag_recv, ag_rs).wait()

    def probs(blk, carry):
        def rows(k):
            return jnp.concatenate([ag_recv[blk * npos + i, k:k + 1, :] for i in range(ndraft)], axis=0)

        m8, r8, a4 = twice(rows(0)), twice(rows(1)), rows(2)
        cols = pl.ds(pl.multiple_of(blk * LANES, LANES), LANES)
        acc_ref[:, cols] = a4
        run, tot = a4[0:1], a4[0:1]
        for i in range(1, ndraft):
            run = run * a4[i:i + 1]
            tot = tot + run
        exp_ref[:, cols] = tot
        for j in range(LANES):
            at = pl.ds(pl.multiple_of((blk * LANES + j) * 8, 8), 8)
            zr[at, :] = jnp.exp(zr[at, :] - m8[:, j:j + 1]) * r8[:, j:j + 1]
        u4 = blk * npos + ndraft
        z4[cols, :] = jnp.exp(z4[cols, :] - to_col(ag_recv[u4, 0:1, :])) * to_col(ag_recv[u4, 1:2, :])
        return carry

    lax.fori_loop(0, nblk, probs, 0)
    bon_copy = pltpu.make_async_copy(z4, bon_ref, out_sem)
    bon_copy.start()

    def excess(g):
        c0, n = CHUNKS[g]

        def body(s, accs):
            new = []
            for c in range(n):
                at = pl.ds(pl.multiple_of((s * per_src + c0 + c) * 8, 8), 8)
                e = jnp.maximum(zr[at, :] - qdst[s, c0 + c], 0.0)
                zr[at, :] = e
                new.append(jnp.where(lane == s, jnp.sum(e, axis=1, keepdims=True), accs[c]))
            return tuple(new)

        accs = lax.fori_loop(0, nd, body, tuple(jnp.zeros((8, LANES), F32) for _ in range(n)), unroll=4)
        for c in range(n):
            zs_send[c0 + c] = accs[c][:4] + accs[c][4:]

    def z_owner(c):
        return (c * 16 + 5) % nd

    def send_sums(g):
        c0, n = CHUNKS[g]
        for c in range(c0, c0 + n):
            @pl.when(me != z_owner(c))
            def _():
                pltpu.make_async_remote_copy(src_ref=zs_send.at[c], dst_ref=zs_recv.at[me], send_sem=zs_ss,
                                             recv_sem=zs_rs, device_id=dev(z_owner(c)), device_id_type=MESH).start()

    def sum_of(ref):
        return lax.fori_loop(0, nd, lambda s, a: a + ref[s], jnp.zeros((4, LANES), F32), unroll=8)

    def own_sums(g):
        c0, n = CHUNKS[g]
        for c in range(c0, c0 + n):
            @pl.when(me == z_owner(c))
            def _():
                pltpu.make_async_copy(zs_send.at[c], zs_recv.at[me], zs_rs).start()
                pltpu.make_async_copy(zs_recv, zs_recv, zs_rs).wait()
                za_send[...] = sum_of(zs_recv)
                pltpu.make_async_copy(za_send, za_recv.at[c], za_rs.at[g]).start()
                each_peer(lambda f: pltpu.make_async_remote_copy(
                    src_ref=za_send, dst_ref=za_recv.at[c], send_sem=za_ss, recv_sem=za_rs.at[g], device_id=dev(f),
                    device_id_type=MESH).start())

    def wait_sums(g):
        c0, n = CHUNKS[g]
        ref = za_recv.at[pl.ds(c0, n)]
        pltpu.make_async_copy(ref, ref, za_rs.at[g]).wait()

    def scale(c, tile):
        r8 = twice(1.0 / tile)
        for s in range(nd):
            at = pl.ds((s * per_src + c) * 8, 8)
            zr[at, :] = zr[at, :] * r8[:, s:s + 1]

    zr4 = zr.reshape(nd, per_src, 8, LANES)

    def put(g):
        c0, n = CHUNKS[g]
        return pltpu.make_async_copy(zr4.at[:, pl.ds(c0, n)], res_ref.at[:, pl.ds(c0, n)], out_sem)

    def finish(g):
        c0, n = CHUNKS[g]

        def one(c, carry):
            scale(c, za_recv[c])
            return carry

        lax.fori_loop(c0, c0 + n, one, 0)
        put(g).start()

    last = len(CHUNKS) - 1
    for g in range(2):
        wait_bulk(g)
        excess(g)
        send_sums(g)
    send_bulk(3)
    for g in range(2):
        own_sums(g)
    wait_bulk(2)
    excess(2)
    send_sums(2)
    own_sums(2)
    for g in range(2):
        wait_sums(g)
        finish(g)
    wait_bulk(last)
    excess(last)
    c_last = CHUNKS[last][0]
    pltpu.make_async_copy(zs_send.at[c_last], zb_recv.at[me], zc_rs).start()
    each_peer(lambda f: pltpu.make_async_remote_copy(
        src_ref=zs_send.at[c_last], dst_ref=zb_recv.at[me], send_sem=zc_ss, recv_sem=zc_rs, device_id=dev(f),
        device_id_type=MESH).start())
    wait_sums(2)
    finish(2)
    pltpu.make_async_copy(zb_recv, zb_recv, zc_rs).wait()
    scale(c_last, sum_of(zb_recv))
    put(last).start()

    def drain(ref, sem):
        pltpu.make_async_copy(ref, ref, sem).wait()

    for g, (c0, n) in enumerate(CHUNKS):
        drain(qsrc.at[pl.ds(c0, n), pl.ds(0, nd - 1)], bulk_ss.at[g])

    @pl.when(is_owner)
    def _():
        drain(st_send.at[pl.ds(0, nunit - 1)], st_ss)
        drain(st_recv.at[pl.ds(0, nd - 1)], ag_ss)

    @pl.when(jnp.logical_not(is_owner))
    def _():
        drain(st_send, st_ss)

    nz = c_last
    is_zowner = (me % 16 == 5) & (me // 16 < nz)

    @pl.when(is_zowner)
    def _():
        drain(zs_send.at[pl.ds(0, nz - 1)], zs_ss)
        drain(st_recv.at[pl.ds(0, nd - 1)], za_ss)

    @pl.when(jnp.logical_not(is_zowner))
    def _():
        drain(zs_send.at[pl.ds(0, nz)], zs_ss)

    drain(st_recv.at[pl.ds(0, nd - 1)], zc_ss)
    bon_copy.wait()
    for g in range(len(CHUNKS)):
        put(g).wait()


def solution(mesh):
    na, nb = mesh.shape["tpa"], mesh.shape["tpb"]
    nd = na * nb

    def local_step(hidden, w_head, q_draft, x_draft):
        nseq, npos, dm = hidden.shape
        ndraft = npos - 1
        vloc = w_head.shape[1]
        per_src = q_draft.shape[0]
        nt = vloc // LANES
        h5 = jnp.transpose(hidden, (1, 0, 2))
        q4 = q_draft.reshape(per_src, ndraft, nd, nt, LANES).transpose(0, 2, 3, 1, 4).reshape(per_src, nd, nt * ndraft,
                                                                                             LANES)
        xt = x_draft.T
        nunit = (nseq // LANES) * npos
        any_ = pl.BlockSpec(memory_space=pl.ANY)
        vmem = pl.BlockSpec(memory_space=pltpu.VMEM)
        dma, vm = pltpu.SemaphoreType.DMA, pltpu.VMEM
        acc, exp, res, bonus = pl.pallas_call(
            functools.partial(kernel, (na, nb)),
            out_shape=[
                jax.ShapeDtypeStruct((ndraft, nseq), F32),
                jax.ShapeDtypeStruct((1, nseq), F32),
                jax.ShapeDtypeStruct((nd, per_src, nt * ndraft, LANES), F32),
                jax.ShapeDtypeStruct((nseq, vloc), F32),
            ],
            in_specs=[any_, any_, any_, vmem],
            out_specs=[vmem, vmem, any_, any_],
            scratch_shapes=[
                vm((NBUF, ROWS, dm), jnp.bfloat16),
                vm((dm, vloc), jnp.bfloat16),
                vm((per_src, nd, 8, LANES), F32),
                vm((nd, per_src, 8, LANES), F32),
                vm((nseq * 8, LANES), F32),
                vm((nseq, vloc), F32),
                vm((ROWS, vloc), F32),
                vm((nunit, 4, LANES), F32),
                vm((nd, 4, LANES), F32),
                vm((4, LANES), F32),
                vm((nunit, 4, LANES), F32),
                vm((per_src, 4, LANES), F32),
                vm((nd, 4, LANES), F32),
                vm((4, LANES), F32),
                vm((per_src, 4, LANES), F32),
                vm((nd, 4, LANES), F32),
                dma((NBUF,)), dma, dma, dma, dma((len(CHUNKS),)), dma((len(CHUNKS),)), dma, dma, dma, dma, dma, dma,
                dma, dma((len(CHUNKS) - 1,)), dma, dma,
            ],
            compiler_params=pltpu.CompilerParams(collective_id=0, has_side_effects=True,
                                                 vmem_limit_bytes=48 * 1024 * 1024),
            name="verify",
        )(h5, w_head, q4, xt)
        residual = res.reshape(nseq, nt, ndraft, LANES).transpose(0, 2, 1, 3).reshape(nseq, ndraft, vloc)
        return acc.T, exp.reshape(nseq), residual, bonus

    return jax.shard_map(
        local_step, mesh=mesh,
        in_specs=(P("dp", None, None), P(None, VOCAB_AXES), P(("dp",) + VOCAB_AXES, None, None), P("dp", None)),
        out_specs=(P("dp", None), P("dp"), P("dp", None, VOCAB_AXES), P("dp", VOCAB_AXES)),
        check_vma=False)
```

```python
import functools

import jax
import jax.numpy as jnp
from jax import lax
from jax.experimental import pallas as pl
from jax.experimental.pallas import tpu as pltpu
from jax.sharding import PartitionSpec as P

INV_TEMP = 1.25
VOCAB_AXES = ("tpa", "tpb")
MESH = pl.DeviceIdType.MESH
F32 = jnp.float32
LANES = 128
CHUNKS = ((0, 4), (4, 1), (5, 2), (7, 1))
ROWS = 256
NBUF = 3


def kernel(dims, h_ref, w_ref, q_ref, xin_ref, acc_ref, exp_ref, zr, z4,
           hbuf, wbuf, x_ref, qsrc, qdst, zb, st_send, st_recv, ag_send, ag_recv, zs_send, zs_recv, za_send, za_recv,
           zb_recv, h_sem, w_sem, q_sem, x_sem, bulk_ss, bulk_rs, st_ss, st_rs, ag_ss, ag_rs, zs_ss, zs_rs, za_ss,
           za_rs, zc_ss, zc_rs):
    na, nb = dims
    nd = na * nb
    me_a, me_b = lax.axis_index("tpa"), lax.axis_index("tpb")
    me = me_a * nb + me_b
    npos = h_ref.shape[0]
    ndraft = npos - 1
    nseq = h_ref.shape[1]
    nblk = nseq // LANES
    nunit = nblk * npos
    per_src = nseq // nd
    vloc = w_ref.shape[1]

    def dev(f):
        return {"tpa": f // nb, "tpb": f % nb}

    px, py, pz = me_b % 4, (me_b // 4) % 4, me_b // 16
    xs = [(px + k) % 4 for k in range(4)]
    ys = [((py + k) % 4) * 4 for k in range(4)]
    cores = [me_a, (me_a + 1) % na]

    def each_peer(fn):
        def plane(kz, carry):
            zz = pz + kz
            base = jnp.where(zz >= 4, zz - 4, zz) * 16
            for ky in range(4):
                for kx in (1, 3, 2, 0):
                    for ka in range(na):
                        b = base + ys[ky] + xs[kx]
                        f = cores[ka] * nb + b
                        ident = {"tpa": cores[ka], "tpb": b}
                        if ka == kx == ky == 0:
                            @pl.when(kz > 0)
                            def _():
                                fn(f, ident)
                        else:
                            fn(f, ident)
            return carry
        lax.fori_loop(0, 4, plane, 0)

    lane = lax.broadcasted_iota(jnp.int32, (8, LANES), 1)
    sub = lax.broadcasted_iota(jnp.int32, (8, LANES), 0)
    sub4 = lax.broadcasted_iota(jnp.int32, (4, LANES), 0)
    lane_f = lane.astype(F32)
    eye = (lax.broadcasted_iota(jnp.int32, (LANES, LANES), 0) == lax.broadcasted_iota(jnp.int32, (LANES, LANES), 1))

    def to_col(row):
        return jnp.sum(jnp.where(eye, jnp.broadcast_to(row, (LANES, LANES)), 0.0), axis=1, keepdims=True)

    def to_row(col):
        return jnp.sum(jnp.where(eye, jnp.broadcast_to(col, (LANES, LANES)), 0.0), axis=0, keepdims=True)

    def twice(t):
        return jnp.concatenate([t, t], axis=0)

    q_copy = pltpu.make_async_copy(q_ref, qsrc, q_sem)
    q_copy.start()
    w_copy = pltpu.make_async_copy(w_ref, wbuf, w_sem)
    w_copy.start()
    per_pos = nseq // ROWS

    def h_copy(t):
        return pltpu.make_async_copy(h_ref.at[t // per_pos, pl.ds((t % per_pos) * ROWS, ROWS)], hbuf.at[t % NBUF],
                                     h_sem.at[t % NBUF])

    x_copy = pltpu.make_async_copy(xin_ref, x_ref, x_sem)
    x_copy.start()
    for t in range(NBUF - 1):
        h_copy(t).start()

    barrier = pltpu.get_barrier_semaphore()
    each_peer(lambda f, ident: pl.semaphore_signal(barrier, inc=1, device_id=ident, device_id_type=MESH))
    q_copy.wait()

    def local_bulk(g):
        c0, n = CHUNKS[g]
        return pltpu.make_async_copy(qsrc.at[pl.ds(c0, n), me], qdst.at[me, pl.ds(c0, n)], bulk_rs.at[g])

    for g in range(len(CHUNKS)):
        local_bulk(g).start()
    pl.semaphore_wait(barrier, nd - 1)

    def send_bulk(g):
        c0, n = CHUNKS[g]

        def one(c, carry):
            each_peer(lambda f, ident: pltpu.make_async_remote_copy(
                src_ref=qsrc.at[c, f], dst_ref=qdst.at[me, c], send_sem=bulk_ss.at[g], recv_sem=bulk_rs.at[g],
                device_id=ident, device_id_type=MESH).start())
            return carry

        lax.fori_loop(c0, c0 + n, one, 0)

    def wait_bulk(g):
        c0, n = CHUNKS[g]
        ref = qdst.at[:, pl.ds(c0, n)]
        pltpu.make_async_copy(ref, ref, bulk_rs.at[g]).wait()

    send_bulk(0)

    x_copy.wait()
    xb = x_ref[:, pl.ds(pl.multiple_of((me // 16) * LANES, LANES), LANES)].astype(F32)
    targets = []
    for c in range(per_src):
        j = (me % 16) * per_src + c
        col = jnp.sum(jnp.where(lane[:4] == j, xb, 0.0), axis=1, keepdims=True)
        targets.append(twice(jnp.broadcast_to(col, (4, LANES))) - jnp.where(sub >= 4, F32(LANES), F32(0)) - lane_f)

    def pick_q(d, accs):
        base = (d * vloc).astype(F32)
        return tuple(a + jnp.where(t == base, qsrc[c, d], 0.0) for c, (a, t) in enumerate(zip(accs, targets)))

    accs = lax.fori_loop(0, nd, pick_q, tuple(jnp.zeros((8, LANES), F32) for _ in range(per_src)))
    qp = jnp.zeros((4, LANES), F32)
    for c in range(per_src):
        col = jnp.sum(accs[c], axis=1, keepdims=True)
        qp = jnp.where(lane[:4] == (me % 16) * per_src + c, col[:4] + col[4:], qp)

    w_copy.wait()
    my_base = (me * vloc).astype(F32)
    lane2 = lax.broadcasted_iota(jnp.int32, (LANES, vloc), 1).astype(F32)

    def matmul(t, carry):
        @pl.when(t + NBUF - 1 < npos * per_pos)
        def _():
            h_copy(t + NBUF - 1).start()

        h_copy(t).wait()
        i, r = t // per_pos, t % per_pos
        zb[...] = jnp.dot(hbuf[t % NBUF], wbuf[...], preferred_element_type=F32) * INV_TEMP
        for half in range(ROWS // LANES):
            blk = r * (ROWS // LANES) + half
            zz = zb[half * LANES:(half + 1) * LANES, :]
            m = jnp.max(zz, axis=1, keepdims=True)
            s = jnp.sum(jnp.exp(zz - m), axis=1, keepdims=True)
            ii = jnp.minimum(i, ndraft - 1)
            xblk = x_ref[:, pl.ds(pl.multiple_of(blk * LANES, LANES), LANES)].astype(F32)
            xrow = jnp.sum(jnp.where(sub4 == ii, xblk, 0.0), axis=0, keepdims=True) - my_base
            pick = jnp.sum(jnp.where(lane2 == to_col(xrow), zz, 0.0), axis=1, keepdims=True)
            qrow = jnp.sum(jnp.where((sub4 == ii) & (blk == me // 16), qp, 0.0), axis=0, keepdims=True)
            tile = jnp.where(sub4 == 0, to_row(m), jnp.where(sub4 == 1, to_row(s), jnp.where(
                sub4 == 2, to_row(pick), qrow)))
            st_send[blk * npos + i] = tile

            @pl.when(i < ndraft)
            def _():
                for lt in range(vloc // LANES):
                    zr[pl.ds(blk * LANES * 8 + lt * 4 + i, LANES, stride=8), :] = zz[:, lt * LANES:(lt + 1) * LANES]

            @pl.when(i == ndraft)
            def _():
                z4[pl.ds(pl.multiple_of(blk * LANES, LANES), LANES), :] = zz
        return carry

    lax.fori_loop(0, npos * per_pos, matmul, 0)

    def owner(u):
        return u * 3

    is_owner = (me % 3 == 0) & (me < nunit * 3)
    my_unit = me // 3

    def send_stats(u, carry):
        f = owner(u)

        @pl.when(f != me)
        def _():
            pltpu.make_async_remote_copy(src_ref=st_send.at[u], dst_ref=st_recv.at[me], send_sem=st_ss, recv_sem=st_rs,
                                         device_id=dev(f), device_id_type=MESH).start()
        return carry

    lax.fori_loop(0, nunit, send_stats, 0)
    send_bulk(1)

    @pl.when(is_owner)
    def _():
        pltpu.make_async_copy(st_send.at[my_unit], st_recv.at[me], st_rs).start()
        pltpu.make_async_copy(st_recv, st_recv, st_rs).wait()
        mx = lax.fori_loop(0, nd, lambda s, m: jnp.maximum(m, st_recv[s]), st_recv[0])[0:1]

        def add(s, carry):
            t = st_recv[s]
            es, zp, qq = carry
            return es + jnp.exp(t[0:1] - mx) * t[1:2], zp + t[2:3], qq + t[3:4]

        zero = jnp.zeros((1, LANES), F32)
        es, zp, qq = lax.fori_loop(0, nd, add, (zero, zero, zero))
        accept = jnp.minimum(1.0, jnp.exp(zp - mx) / es / qq)
        ag_send[...] = jnp.where(sub4 == 0, mx, jnp.where(sub4 == 1, 1.0 / es, accept))
        pltpu.make_async_copy(ag_send, ag_recv.at[my_unit], ag_rs).start()
        each_peer(lambda f, ident: pltpu.make_async_remote_copy(
            src_ref=ag_send, dst_ref=ag_recv.at[my_unit], send_sem=ag_ss, recv_sem=ag_rs, device_id=ident,
            device_id_type=MESH).start())

    send_bulk(2)

    pltpu.make_async_copy(ag_recv, ag_recv, ag_rs).wait()

    def probs(blk, carry):
        def rows(k):
            return jnp.concatenate([ag_recv[blk * npos + i, k:k + 1, :] for i in range(ndraft)], axis=0)

        m8, r8, a4 = twice(rows(0)), twice(rows(1)), rows(2)
        cols = pl.ds(pl.multiple_of(blk * LANES, LANES), LANES)
        acc_ref[:, cols] = a4
        run, tot = a4[0:1], a4[0:1]
        for i in range(1, ndraft):
            run = run * a4[i:i + 1]
            tot = tot + run
        exp_ref[:, cols] = tot
        for j in range(LANES):
            at = pl.ds(pl.multiple_of((blk * LANES + j) * 8, 8), 8)
            zr[at, :] = jnp.exp(zr[at, :] - m8[:, j:j + 1]) * r8[:, j:j + 1]
        u4 = blk * npos + ndraft
        z4[cols, :] = jnp.exp(z4[cols, :] - to_col(ag_recv[u4, 0:1, :])) * to_col(ag_recv[u4, 1:2, :])
        return carry

    lax.fori_loop(0, nblk, probs, 0)

    def excess(g):
        c0, n = CHUNKS[g]

        def body(s, accs):
            new = []
            for c in range(n):
                at = pl.ds(pl.multiple_of((s * per_src + c0 + c) * 8, 8), 8)
                e = jnp.maximum(zr[at, :] - qdst[s, c0 + c], 0.0)
                zr[at, :] = e
                new.append(jnp.where(lane == s, jnp.sum(e, axis=1, keepdims=True), accs[c]))
            return tuple(new)

        accs = lax.fori_loop(0, nd, body, tuple(jnp.zeros((8, LANES), F32) for _ in range(n)), unroll=4)
        for c in range(n):
            zs_send[c0 + c] = accs[c][:4] + accs[c][4:]

    def z_owner(c):
        return (c * 16 + 5) % nd

    def send_sums(g):
        c0, n = CHUNKS[g]
        for c in range(c0, c0 + n):
            @pl.when(me != z_owner(c))
            def _():
                pltpu.make_async_remote_copy(src_ref=zs_send.at[c], dst_ref=zs_recv.at[me], send_sem=zs_ss,
                                             recv_sem=zs_rs, device_id=dev(z_owner(c)), device_id_type=MESH).start()

    def sum_of(ref):
        return lax.fori_loop(0, nd, lambda s, a: a + ref[s], jnp.zeros((4, LANES), F32), unroll=8)

    def own_sums(g):
        c0, n = CHUNKS[g]
        for c in range(c0, c0 + n):
            @pl.when(me == z_owner(c))
            def _():
                pltpu.make_async_copy(zs_send.at[c], zs_recv.at[me], zs_rs).start()
                pltpu.make_async_copy(zs_recv, zs_recv, zs_rs).wait()
                za_send[...] = sum_of(zs_recv)
                pltpu.make_async_copy(za_send, za_recv.at[c], za_rs.at[g]).start()
                each_peer(lambda f, ident: pltpu.make_async_remote_copy(
                    src_ref=za_send, dst_ref=za_recv.at[c], send_sem=za_ss, recv_sem=za_rs.at[g], device_id=ident,
                    device_id_type=MESH).start())

    def wait_sums(g):
        c0, n = CHUNKS[g]
        ref = za_recv.at[pl.ds(c0, n)]
        pltpu.make_async_copy(ref, ref, za_rs.at[g]).wait()

    def scale(c, tile):
        r8 = twice(1.0 / tile)
        for s in range(nd):
            at = pl.ds((s * per_src + c) * 8, 8)
            zr[at, :] = zr[at, :] * r8[:, s:s + 1]

    def finish(g):
        c0, n = CHUNKS[g]

        def one(c, carry):
            scale(c, za_recv[c])
            return carry

        lax.fori_loop(c0, c0 + n, one, 0)

    last = len(CHUNKS) - 1
    for g in range(2):
        wait_bulk(g)
        excess(g)
        send_sums(g)
    send_bulk(3)
    for g in range(2):
        own_sums(g)
    wait_bulk(2)
    excess(2)
    send_sums(2)
    own_sums(2)
    for g in range(2):
        wait_sums(g)
        finish(g)
    wait_bulk(last)
    excess(last)
    c_last = CHUNKS[last][0]
    pltpu.make_async_copy(zs_send.at[c_last], zb_recv.at[me], zc_rs).start()
    each_peer(lambda f, ident: pltpu.make_async_remote_copy(
        src_ref=zs_send.at[c_last], dst_ref=zb_recv.at[me], send_sem=zc_ss, recv_sem=zc_rs, device_id=ident,
        device_id_type=MESH).start())
    wait_sums(2)
    finish(2)
    pltpu.make_async_copy(zb_recv, zb_recv, zc_rs).wait()
    scale(c_last, sum_of(zb_recv))

    def drain(ref, sem):
        pltpu.make_async_copy(ref, ref, sem).wait()

    for g, (c0, n) in enumerate(CHUNKS):
        drain(qsrc.at[pl.ds(c0, n), pl.ds(0, nd - 1)], bulk_ss.at[g])

    @pl.when(is_owner)
    def _():
        drain(st_send.at[pl.ds(0, nunit - 1)], st_ss)
        drain(st_recv.at[pl.ds(0, nd - 1)], ag_ss)

    @pl.when(jnp.logical_not(is_owner))
    def _():
        drain(st_send, st_ss)

    nz = c_last
    is_zowner = (me % 16 == 5) & (me // 16 < nz)

    @pl.when(is_zowner)
    def _():
        drain(zs_send.at[pl.ds(0, nz - 1)], zs_ss)
        drain(st_recv.at[pl.ds(0, nd - 1)], za_ss)

    @pl.when(jnp.logical_not(is_zowner))
    def _():
        drain(zs_send.at[pl.ds(0, nz)], zs_ss)

    drain(st_recv.at[pl.ds(0, nd - 1)], zc_ss)


def write_out(*refs):
    copies = [pltpu.make_async_copy(refs[k], refs[4 + k], refs[8].at[k]) for k in range(4)]
    for c in copies:
        c.start()
    for c in copies:
        c.wait()


def solution(mesh):
    na, nb = mesh.shape["tpa"], mesh.shape["tpb"]
    nd = na * nb

    def local_step(hidden, w_head, q_draft, x_draft):
        nseq, npos, dm = hidden.shape
        ndraft = npos - 1
        vloc = w_head.shape[1]
        per_src = q_draft.shape[0]
        nt = vloc // LANES
        h5 = jnp.transpose(hidden, (1, 0, 2))
        q4 = q_draft.reshape(per_src, ndraft, nd, nt, LANES).transpose(0, 2, 3, 1, 4).reshape(per_src, nd, nt * ndraft,
                                                                                             LANES)
        xt = x_draft.T
        nunit = (nseq // LANES) * npos
        hbm = pl.BlockSpec(memory_space=pltpu.HBM)
        vmem = pl.BlockSpec(memory_space=pltpu.VMEM)
        dma, vm = pltpu.SemaphoreType.DMA, pltpu.VMEM
        outs = pl.pallas_call(
            functools.partial(kernel, (na, nb)),
            out_shape=[
                jax.ShapeDtypeStruct((ndraft, nseq), F32),
                jax.ShapeDtypeStruct((1, nseq), F32),
                jax.ShapeDtypeStruct((nseq * nt * ndraft, LANES), F32),
                jax.ShapeDtypeStruct((nseq, vloc), F32),
            ],
            in_specs=[hbm] * 4,
            out_specs=[vmem] * 4,
            scratch_shapes=[
                vm((NBUF, ROWS, dm), jnp.bfloat16),
                vm((dm, vloc), jnp.bfloat16),
                vm((ndraft, nseq), jnp.int32),
                vm((per_src, nd, 8, LANES), F32),
                vm((nd, per_src, 8, LANES), F32),
                vm((ROWS, vloc), F32),
                vm((nunit, 4, LANES), F32),
                vm((nd, 4, LANES), F32),
                vm((4, LANES), F32),
                vm((nunit, 4, LANES), F32),
                vm((per_src, 4, LANES), F32),
                vm((nd, 4, LANES), F32),
                vm((4, LANES), F32),
                vm((per_src, 4, LANES), F32),
                vm((nd, 4, LANES), F32),
                dma((NBUF,)), dma, dma, dma, dma((len(CHUNKS),)), dma((len(CHUNKS),)), dma, dma, dma, dma, dma, dma,
                dma, dma((len(CHUNKS) - 1,)), dma, dma,
            ],
            compiler_params=pltpu.CompilerParams(collective_id=0, has_side_effects=True,
                                                 vmem_limit_bytes=46 * 1024 * 1024),
            name="verify",
        )(*[pltpu.with_memory_space_constraint(a, pltpu.HBM) for a in (h5, w_head, q4, xt)])
        acc, exp, res, bonus = pl.pallas_call(
            write_out,
            out_shape=[jax.ShapeDtypeStruct(o.shape, o.dtype) for o in outs],
            in_specs=[vmem] * 4,
            out_specs=[hbm] * 4,
            scratch_shapes=[dma((4,))],
            compiler_params=pltpu.CompilerParams(vmem_limit_bytes=4 * 1024 * 1024),
            name="write_out",
        )(*outs)
        residual = res.reshape(nseq, nt, ndraft, LANES).transpose(0, 2, 1, 3).reshape(nseq, ndraft, vloc)
        return acc.T, exp.reshape(nseq), residual, bonus

    return jax.shard_map(
        local_step, mesh=mesh,
        in_specs=(P("dp", None, None), P(None, VOCAB_AXES), P(("dp",) + VOCAB_AXES, None, None), P("dp", None)),
        out_specs=(P("dp", None), P("dp"), P("dp", None, VOCAB_AXES), P("dp", VOCAB_AXES)),
        check_vma=False)
```

```python
import functools

import jax
import jax.numpy as jnp
from jax import lax
from jax.experimental import pallas as pl
from jax.experimental.pallas import tpu as pltpu
from jax.sharding import PartitionSpec as P

INV_TEMP = 1.25
VOCAB_AXES = ("tpa", "tpb")
MESH = pl.DeviceIdType.MESH
F32 = jnp.float32
LANES = 128
CHUNKS = ((0, 3), (3, 1), (4, 3), (7, 1))
ROWS = 256
NBUF = 3


def kernel(dims, h_ref, w_ref, q_ref, xin_ref, acc_ref, exp_ref, zr, z4,
           hbuf, wbuf, x_ref, qsrc, qdst, zb, st_send, st_recv, ag_send, ag_recv, zs_send, zs_recv, za_send, za_recv,
           zb_recv, h_sem, w_sem, q_sem, x_sem, bulk_ss, bulk_rs, st_ss, st_rs, ag_ss, ag_rs, zs_ss, zs_rs, za_ss,
           za_rs, zc_ss, zc_rs):
    na, nb = dims
    nd = na * nb
    me_a, me_b = lax.axis_index("tpa"), lax.axis_index("tpb")
    me = me_a * nb + me_b
    npos = h_ref.shape[0]
    ndraft = npos - 1
    nseq = h_ref.shape[1]
    nblk = nseq // LANES
    nunit = nblk * npos
    per_src = nseq // nd
    vloc = w_ref.shape[1]

    def dev(f):
        return {"tpa": f // nb, "tpb": f % nb}

    px, py, pz = me_b % 4, (me_b // 4) % 4, me_b // 16
    xs = [(px + k) % 4 for k in range(4)]
    ys = [((py + k) % 4) * 4 for k in range(4)]
    cores = [me_a, (me_a + 1) % na]

    def each_peer(fn, far=False):
        first = 2 if far else 0

        def plane(kz, carry):
            zz = pz + kz + first
            zz = jnp.where(zz >= 4, zz - 4, zz)
            base = jnp.where(zz >= 4, zz - 4, zz) * 16
            for ky in (2, 1, 3, 0) if far else range(4):
                for kx in (2, 1, 3, 0) if far else (1, 3, 2, 0):
                    for ka in range(na):
                        b = base + ys[ky] + xs[kx]
                        f = cores[ka] * nb + b
                        ident = {"tpa": cores[ka], "tpb": b}
                        if ka == kx == ky == 0:
                            @pl.when(kz != (4 - first) % 4)
                            def _():
                                fn(f, ident)
                        else:
                            fn(f, ident)
            return carry
        lax.fori_loop(0, 4, plane, 0)

    lane = lax.broadcasted_iota(jnp.int32, (8, LANES), 1)
    sub = lax.broadcasted_iota(jnp.int32, (8, LANES), 0)
    sub4 = lax.broadcasted_iota(jnp.int32, (4, LANES), 0)
    lane_f = lane.astype(F32)
    eye = (lax.broadcasted_iota(jnp.int32, (LANES, LANES), 0) == lax.broadcasted_iota(jnp.int32, (LANES, LANES), 1))

    def to_col(row):
        return jnp.sum(jnp.where(eye, jnp.broadcast_to(row, (LANES, LANES)), 0.0), axis=1, keepdims=True)

    def to_row(col):
        return jnp.sum(jnp.where(eye, jnp.broadcast_to(col, (LANES, LANES)), 0.0), axis=0, keepdims=True)

    def twice(t):
        return jnp.concatenate([t, t], axis=0)

    q_copy = pltpu.make_async_copy(q_ref, qsrc, q_sem)
    q_copy.start()
    w_copy = pltpu.make_async_copy(w_ref, wbuf, w_sem)
    w_copy.start()
    per_pos = nseq // ROWS

    def h_copy(t):
        return pltpu.make_async_copy(h_ref.at[t // per_pos, pl.ds((t % per_pos) * ROWS, ROWS)], hbuf.at[t % NBUF],
                                     h_sem.at[t % NBUF])

    x_copy = pltpu.make_async_copy(xin_ref, x_ref, x_sem)
    x_copy.start()
    for t in range(NBUF - 1):
        h_copy(t).start()

    barrier = pltpu.get_barrier_semaphore()
    each_peer(lambda f, ident: pl.semaphore_signal(barrier, inc=1, device_id=ident, device_id_type=MESH), far=True)
    q_copy.wait()

    def local_bulk(g):
        c0, n = CHUNKS[g]
        return pltpu.make_async_copy(qsrc.at[pl.ds(c0, n), me], qdst.at[me, pl.ds(c0, n)], bulk_rs.at[g])

    for g in range(len(CHUNKS)):
        local_bulk(g).start()
    x_copy.wait()
    xb = x_ref[:, pl.ds(pl.multiple_of((me // 16) * LANES, LANES), LANES)].astype(F32)
    targets = []
    for c in range(per_src):
        j = (me % 16) * per_src + c
        col = jnp.sum(jnp.where(lane[:4] == j, xb, 0.0), axis=1, keepdims=True)
        targets.append(twice(jnp.broadcast_to(col, (4, LANES))) - jnp.where(sub >= 4, F32(LANES), F32(0)) - lane_f)

    def pick_q(d, accs):
        base = (d * vloc).astype(F32)
        return tuple(a + jnp.where(t == base, qsrc[c, d], 0.0) for c, (a, t) in enumerate(zip(accs, targets)))

    accs = lax.fori_loop(0, nd, pick_q, tuple(jnp.zeros((8, LANES), F32) for _ in range(per_src)))
    qp = jnp.zeros((4, LANES), F32)
    for c in range(per_src):
        col = jnp.sum(accs[c], axis=1, keepdims=True)
        qp = jnp.where(lane[:4] == (me % 16) * per_src + c, col[:4] + col[4:], qp)

    pl.semaphore_wait(barrier, nd - 1)

    def send_bulk(g):
        c0, n = CHUNKS[g]

        def one(c, carry):
            each_peer(lambda f, ident: pltpu.make_async_remote_copy(
                src_ref=qsrc.at[c, f], dst_ref=qdst.at[me, c], send_sem=bulk_ss.at[g], recv_sem=bulk_rs.at[g],
                device_id=ident, device_id_type=MESH).start())
            return carry

        lax.fori_loop(c0, c0 + n, one, 0)

    def wait_bulk(g):
        c0, n = CHUNKS[g]
        ref = qdst.at[:, pl.ds(c0, n)]
        pltpu.make_async_copy(ref, ref, bulk_rs.at[g]).wait()

    send_bulk(0)

    w_copy.wait()
    my_base = (me * vloc).astype(F32)
    lane2 = lax.broadcasted_iota(jnp.int32, (LANES, vloc), 1).astype(F32)

    def matmul(t, carry):
        @pl.when(t + NBUF - 1 < npos * per_pos)
        def _():
            h_copy(t + NBUF - 1).start()

        h_copy(t).wait()
        i, r = t // per_pos, t % per_pos
        zb[...] = jnp.dot(hbuf[t % NBUF], wbuf[...], preferred_element_type=F32) * INV_TEMP
        for half in range(ROWS // LANES):
            blk = r * (ROWS // LANES) + half
            zz = zb[half * LANES:(half + 1) * LANES, :]
            m = jnp.max(zz, axis=1, keepdims=True)
            s = jnp.sum(jnp.exp(zz - m), axis=1, keepdims=True)
            ii = jnp.minimum(i, ndraft - 1)
            xblk = x_ref[:, pl.ds(pl.multiple_of(blk * LANES, LANES), LANES)].astype(F32)
            xrow = jnp.sum(jnp.where(sub4 == ii, xblk, 0.0), axis=0, keepdims=True) - my_base
            pick = jnp.sum(jnp.where(lane2 == to_col(xrow), zz, 0.0), axis=1, keepdims=True)
            qrow = jnp.sum(jnp.where((sub4 == ii) & (blk == me // 16), qp, 0.0), axis=0, keepdims=True)
            tile = jnp.where(sub4 == 0, to_row(m), jnp.where(sub4 == 1, to_row(s), jnp.where(
                sub4 == 2, to_row(pick), qrow)))
            st_send[blk * npos + i] = tile

            @pl.when(i < ndraft)
            def _():
                for lt in range(vloc // LANES):
                    zr[pl.ds(blk * LANES * 8 + lt * 4 + i, LANES, stride=8), :] = zz[:, lt * LANES:(lt + 1) * LANES]

            @pl.when(i == ndraft)
            def _():
                z4[pl.ds(pl.multiple_of(blk * LANES, LANES), LANES), :] = zz
        return carry

    lax.fori_loop(0, npos * per_pos, matmul, 0)

    def owner(u):
        return u * 3

    is_owner = (me % 3 == 0) & (me < nunit * 3)
    my_unit = me // 3

    def send_stats(u, carry):
        f = owner(u)

        @pl.when(f != me)
        def _():
            pltpu.make_async_remote_copy(src_ref=st_send.at[u], dst_ref=st_recv.at[me], send_sem=st_ss, recv_sem=st_rs,
                                         device_id=dev(f), device_id_type=MESH).start()
        return carry

    lax.fori_loop(0, nunit, send_stats, 0)
    send_bulk(1)

    @pl.when(is_owner)
    def _():
        pltpu.make_async_copy(st_send.at[my_unit], st_recv.at[me], st_rs).start()
        pltpu.make_async_copy(st_recv, st_recv, st_rs).wait()
        mx = lax.fori_loop(0, nd, lambda s, m: jnp.maximum(m, st_recv[s]), st_recv[0])[0:1]

        def add(s, carry):
            t = st_recv[s]
            es, zp, qq = carry
            return es + jnp.exp(t[0:1] - mx) * t[1:2], zp + t[2:3], qq + t[3:4]

        zero = jnp.zeros((1, LANES), F32)
        es, zp, qq = lax.fori_loop(0, nd, add, (zero, zero, zero))
        accept = jnp.minimum(1.0, jnp.exp(zp - mx) / es / qq)
        ag_send[...] = jnp.where(sub4 == 0, mx, jnp.where(sub4 == 1, 1.0 / es, accept))
        pltpu.make_async_copy(ag_send, ag_recv.at[my_unit], ag_rs).start()
        each_peer(lambda f, ident: pltpu.make_async_remote_copy(
            src_ref=ag_send, dst_ref=ag_recv.at[my_unit], send_sem=ag_ss, recv_sem=ag_rs, device_id=ident,
            device_id_type=MESH).start(), far=True)

    send_bulk(2)

    pltpu.make_async_copy(ag_recv, ag_recv, ag_rs).wait()

    def stat_rows(blk, k):
        return jnp.concatenate([ag_recv[blk * npos + i, k:k + 1, :] for i in range(ndraft)], axis=0)

    def probs(c0, n):
        def body(blk, carry):
            m8, r8 = twice(stat_rows(blk, 0)), twice(stat_rows(blk, 1))
            for j in range(LANES):
                if c0 <= j % per_src < c0 + n:
                    at = pl.ds(pl.multiple_of((blk * LANES + j) * 8, 8), 8)
                    zr[at, :] = jnp.exp(zr[at, :] - m8[:, j:j + 1]) * r8[:, j:j + 1]
            return carry
        lax.fori_loop(0, nblk, body, 0)

    def verdicts(blk, carry):
        a4 = stat_rows(blk, 2)
        cols = pl.ds(pl.multiple_of(blk * LANES, LANES), LANES)
        acc_ref[:, cols] = a4
        run, tot = a4[0:1], a4[0:1]
        for i in range(1, ndraft):
            run = run * a4[i:i + 1]
            tot = tot + run
        exp_ref[:, cols] = tot
        u4 = blk * npos + ndraft
        z4[cols, :] = jnp.exp(z4[cols, :] - to_col(ag_recv[u4, 0:1, :])) * to_col(ag_recv[u4, 1:2, :])
        return carry

    def excess(g):
        c0, n = CHUNKS[g]

        def body(s, accs):
            new = []
            for c in range(n):
                at = pl.ds(pl.multiple_of((s * per_src + c0 + c) * 8, 8), 8)
                e = jnp.maximum(zr[at, :] - qdst[s, c0 + c], 0.0)
                zr[at, :] = e
                new.append(jnp.where(lane == s, jnp.sum(e, axis=1, keepdims=True), accs[c]))
            return tuple(new)

        accs = lax.fori_loop(0, nd, body, tuple(jnp.zeros((8, LANES), F32) for _ in range(n)), unroll=4)
        for c in range(n):
            zs_send[c0 + c] = accs[c][:4] + accs[c][4:]

    def z_owner(c):
        return (c * 16 + 5) % nd

    def send_sums(g):
        c0, n = CHUNKS[g]
        for c in range(c0, c0 + n):
            @pl.when(me != z_owner(c))
            def _():
                pltpu.make_async_remote_copy(src_ref=zs_send.at[c], dst_ref=zs_recv.at[me], send_sem=zs_ss,
                                             recv_sem=zs_rs, device_id=dev(z_owner(c)), device_id_type=MESH).start()

    def sum_of(ref):
        return lax.fori_loop(0, nd, lambda s, a: a + ref[s], jnp.zeros((4, LANES), F32), unroll=8)

    def own_sums(g):
        c0, n = CHUNKS[g]
        for c in range(c0, c0 + n):
            @pl.when(me == z_owner(c))
            def _():
                pltpu.make_async_copy(zs_send.at[c], zs_recv.at[me], zs_rs).start()
                pltpu.make_async_copy(zs_recv, zs_recv, zs_rs).wait()
                za_send[...] = sum_of(zs_recv)
                pltpu.make_async_copy(za_send, za_recv.at[c], za_rs.at[g]).start()
                each_peer(lambda f, ident: pltpu.make_async_remote_copy(
                    src_ref=za_send, dst_ref=za_recv.at[c], send_sem=za_ss, recv_sem=za_rs.at[g], device_id=ident,
                    device_id_type=MESH).start(), far=True)

    def wait_sums(g):
        c0, n = CHUNKS[g]
        ref = za_recv.at[pl.ds(c0, n)]
        pltpu.make_async_copy(ref, ref, za_rs.at[g]).wait()

    def scale(c, tile):
        r8 = twice(1.0 / tile)
        for s in range(nd):
            at = pl.ds((s * per_src + c) * 8, 8)
            zr[at, :] = zr[at, :] * r8[:, s:s + 1]

    def finish(g):
        c0, n = CHUNKS[g]

        def one(c, carry):
            scale(c, za_recv[c])
            return carry

        lax.fori_loop(c0, c0 + n, one, 0)

    last = len(CHUNKS) - 1
    half = CHUNKS[2][0]
    probs(0, half)
    for g in range(2):
        wait_bulk(g)
        excess(g)
        send_sums(g)
    send_bulk(3)
    probs(half, per_src - half)
    for g in range(2):
        own_sums(g)
    wait_bulk(2)
    excess(2)
    send_sums(2)
    lax.fori_loop(0, nblk, verdicts, 0)
    own_sums(2)
    for g in range(2):
        wait_sums(g)
        finish(g)
    wait_bulk(last)
    excess(last)
    c_last = CHUNKS[last][0]
    pltpu.make_async_copy(zs_send.at[c_last], zb_recv.at[me], zc_rs).start()
    each_peer(lambda f, ident: pltpu.make_async_remote_copy(
        src_ref=zs_send.at[c_last], dst_ref=zb_recv.at[me], send_sem=zc_ss, recv_sem=zc_rs, device_id=ident,
        device_id_type=MESH).start(), far=True)
    wait_sums(2)
    finish(2)
    pltpu.make_async_copy(zb_recv, zb_recv, zc_rs).wait()
    scale(c_last, sum_of(zb_recv))

    def drain(ref, sem):
        pltpu.make_async_copy(ref, ref, sem).wait()

    for g, (c0, n) in enumerate(CHUNKS):
        drain(qsrc.at[pl.ds(c0, n), pl.ds(0, nd - 1)], bulk_ss.at[g])

    @pl.when(is_owner)
    def _():
        drain(st_send.at[pl.ds(0, nunit - 1)], st_ss)
        drain(st_recv.at[pl.ds(0, nd - 1)], ag_ss)

    @pl.when(jnp.logical_not(is_owner))
    def _():
        drain(st_send, st_ss)

    nz = c_last
    is_zowner = (me % 16 == 5) & (me // 16 < nz)

    @pl.when(is_zowner)
    def _():
        drain(zs_send.at[pl.ds(0, nz - 1)], zs_ss)
        drain(st_recv.at[pl.ds(0, nd - 1)], za_ss)

    @pl.when(jnp.logical_not(is_zowner))
    def _():
        drain(zs_send.at[pl.ds(0, nz)], zs_ss)

    drain(st_recv.at[pl.ds(0, nd - 1)], zc_ss)


def write_out(*refs):
    copies = [pltpu.make_async_copy(refs[k], refs[4 + k], refs[8].at[k]) for k in range(4)]
    for c in copies:
        c.start()
    for c in copies:
        c.wait()


def solution(mesh):
    na, nb = mesh.shape["tpa"], mesh.shape["tpb"]
    nd = na * nb

    def local_step(hidden, w_head, q_draft, x_draft):
        nseq, npos, dm = hidden.shape
        ndraft = npos - 1
        vloc = w_head.shape[1]
        per_src = q_draft.shape[0]
        nt = vloc // LANES
        h5 = jnp.transpose(hidden, (1, 0, 2))
        q4 = q_draft.reshape(per_src, ndraft, nd, nt, LANES).transpose(0, 2, 3, 1, 4).reshape(per_src, nd, nt * ndraft,
                                                                                             LANES)
        xt = x_draft.T
        nunit = (nseq // LANES) * npos
        hbm = pl.BlockSpec(memory_space=pltpu.HBM)
        vmem = pl.BlockSpec(memory_space=pltpu.VMEM)
        dma, vm = pltpu.SemaphoreType.DMA, pltpu.VMEM
        outs = pl.pallas_call(
            functools.partial(kernel, (na, nb)),
            out_shape=[
                jax.ShapeDtypeStruct((ndraft, nseq), F32),
                jax.ShapeDtypeStruct((1, nseq), F32),
                jax.ShapeDtypeStruct((nseq * nt * ndraft, LANES), F32),
                jax.ShapeDtypeStruct((nseq, vloc), F32),
            ],
            in_specs=[hbm] * 4,
            out_specs=[vmem] * 4,
            scratch_shapes=[
                vm((NBUF, ROWS, dm), jnp.bfloat16),
                vm((dm, vloc), jnp.bfloat16),
                vm((ndraft, nseq), jnp.int32),
                vm((per_src, nd, 8, LANES), F32),
                vm((nd, per_src, 8, LANES), F32),
                vm((ROWS, vloc), F32),
                vm((nunit, 4, LANES), F32),
                vm((nd, 4, LANES), F32),
                vm((4, LANES), F32),
                vm((nunit, 4, LANES), F32),
                vm((per_src, 4, LANES), F32),
                vm((nd, 4, LANES), F32),
                vm((4, LANES), F32),
                vm((per_src, 4, LANES), F32),
                vm((nd, 4, LANES), F32),
                dma((NBUF,)), dma, dma, dma, dma((len(CHUNKS),)), dma((len(CHUNKS),)), dma, dma, dma, dma, dma, dma,
                dma, dma((len(CHUNKS) - 1,)), dma, dma,
            ],
            compiler_params=pltpu.CompilerParams(collective_id=0, has_side_effects=True,
                                                 vmem_limit_bytes=46 * 1024 * 1024),
            name="verify",
        )(*[pltpu.with_memory_space_constraint(a, pltpu.HBM) for a in (h5, w_head, q4, xt)])
        acc, exp, res, bonus = pl.pallas_call(
            write_out,
            out_shape=[jax.ShapeDtypeStruct(o.shape, o.dtype) for o in outs],
            in_specs=[vmem] * 4,
            out_specs=[hbm] * 4,
            scratch_shapes=[dma((4,))],
            compiler_params=pltpu.CompilerParams(vmem_limit_bytes=4 * 1024 * 1024),
            name="write_out",
        )(*outs)
        residual = res.reshape(nseq, nt, ndraft, LANES).transpose(0, 2, 1, 3).reshape(nseq, ndraft, vloc)
        return acc.T, exp.reshape(nseq), residual, bonus

    return jax.shard_map(
        local_step, mesh=mesh,
        in_specs=(P("dp", None, None), P(None, VOCAB_AXES), P(("dp",) + VOCAB_AXES, None, None), P("dp", None)),
        out_specs=(P("dp", None), P("dp"), P("dp", None, VOCAB_AXES), P("dp", VOCAB_AXES)),
        check_vma=False)
```

```python
import functools

import jax
import jax.numpy as jnp
from jax import lax
from jax.experimental import pallas as pl
from jax.experimental.pallas import tpu as pltpu
from jax.sharding import PartitionSpec as P

INV_TEMP = 1.25
VOCAB_AXES = ("tpa", "tpb")
MESH = pl.DeviceIdType.MESH
F32 = jnp.float32
LANES = 128
CHUNKS = ((0, 3), (3, 1), (4, 2), (6, 1), (7, 1))
ROWS = 256
NBUF = 3
EARLY = 3


def kernel(dims, h_ref, w_ref, q_ref, xin_ref, acc_ref, exp_ref, zr, z4, rz_ref,
           hbuf, wbuf, x_ref, qsrc, qdst, zb, st_send, st_recv, ag_send, ag_recv, zs_send, zs_recv, h_sem, w_sem, q_sem,
           x_sem, bulk_ss, bulk_rs, st_ss, st_rs, ag_ss, ag_rs, zs_ss, zs_rs):
    na, nb = dims
    nd = na * nb
    me_a, me_b = lax.axis_index("tpa"), lax.axis_index("tpb")
    me = me_a * nb + me_b
    npos = h_ref.shape[0]
    ndraft = npos - 1
    nseq = h_ref.shape[1]
    nblk = nseq // LANES
    nunit = nblk * npos
    per_src = nseq // nd
    vloc = w_ref.shape[1]

    def dev(f):
        return {"tpa": f // nb, "tpb": f % nb}

    px, py, pz = me_b % 4, (me_b // 4) % 4, me_b // 16
    xs = [(px + k) % 4 for k in range(4)]
    ys = [((py + k) % 4) * 4 for k in range(4)]
    cores = [me_a, (me_a + 1) % na]

    def each_peer(fn, far=False):
        first = 2 if far else 0

        def plane(kz, carry):
            zz = pz + kz + first
            zz = jnp.where(zz >= 4, zz - 4, zz)
            base = jnp.where(zz >= 4, zz - 4, zz) * 16
            for ky in (2, 1, 3, 0) if far else range(4):
                for kx in (2, 1, 3, 0) if far else (1, 3, 2, 0):
                    for ka in range(na):
                        b = base + ys[ky] + xs[kx]
                        f = cores[ka] * nb + b
                        ident = {"tpa": cores[ka], "tpb": b}
                        if ka == kx == ky == 0:
                            @pl.when(kz != (4 - first) % 4)
                            def _():
                                fn(f, ident)
                        else:
                            fn(f, ident)
            return carry
        lax.fori_loop(0, 4, plane, 0)

    lane = lax.broadcasted_iota(jnp.int32, (8, LANES), 1)
    sub = lax.broadcasted_iota(jnp.int32, (8, LANES), 0)
    sub4 = lax.broadcasted_iota(jnp.int32, (4, LANES), 0)
    lane_f = lane.astype(F32)
    eye = (lax.broadcasted_iota(jnp.int32, (LANES, LANES), 0) == lax.broadcasted_iota(jnp.int32, (LANES, LANES), 1))

    def to_col(row):
        return jnp.sum(jnp.where(eye, jnp.broadcast_to(row, (LANES, LANES)), 0.0), axis=1, keepdims=True)

    def to_row(col):
        return jnp.sum(jnp.where(eye, jnp.broadcast_to(col, (LANES, LANES)), 0.0), axis=0, keepdims=True)

    def twice(t):
        return jnp.concatenate([t, t], axis=0)

    q_copy = pltpu.make_async_copy(q_ref, qsrc, q_sem)
    q_copy.start()
    w_copy = pltpu.make_async_copy(w_ref, wbuf, w_sem)
    w_copy.start()
    per_pos = nseq // ROWS

    def h_copy(t):
        return pltpu.make_async_copy(h_ref.at[t // per_pos, pl.ds((t % per_pos) * ROWS, ROWS)], hbuf.at[t % NBUF],
                                     h_sem.at[t % NBUF])

    x_copy = pltpu.make_async_copy(xin_ref, x_ref, x_sem)
    x_copy.start()
    for t in range(NBUF - 1):
        h_copy(t).start()

    barrier = pltpu.get_barrier_semaphore()
    each_peer(lambda f, ident: pl.semaphore_signal(barrier, inc=1, device_id=ident, device_id_type=MESH), far=True)
    q_copy.wait()

    def local_bulk(g):
        c0, n = CHUNKS[g]
        return pltpu.make_async_copy(qsrc.at[pl.ds(c0, n), me], qdst.at[me, pl.ds(c0, n)], bulk_rs.at[g])

    for g in range(len(CHUNKS)):
        local_bulk(g).start()
    x_copy.wait()
    xb = x_ref[:, pl.ds(pl.multiple_of((me // 16) * LANES, LANES), LANES)].astype(F32)
    targets = []
    for c in range(per_src):
        j = (me % 16) * per_src + c
        col = jnp.sum(jnp.where(lane[:4] == j, xb, 0.0), axis=1, keepdims=True)
        targets.append(twice(jnp.broadcast_to(col, (4, LANES))) - jnp.where(sub >= 4, F32(LANES), F32(0)) - lane_f)

    def pick_q(d, accs):
        base = (d * vloc).astype(F32)
        return tuple(a + jnp.where(t == base, qsrc[c, d], 0.0) for c, (a, t) in enumerate(zip(accs, targets)))

    accs = lax.fori_loop(0, nd, pick_q, tuple(jnp.zeros((8, LANES), F32) for _ in range(per_src)),
                         unroll=8)
    qp = jnp.zeros((4, LANES), F32)
    for c in range(per_src):
        col = jnp.sum(accs[c], axis=1, keepdims=True)
        qp = jnp.where(lane[:4] == (me % 16) * per_src + c, col[:4] + col[4:], qp)


    def send_bulk(g):
        c0, n = CHUNKS[g]

        def one(c, carry):
            each_peer(lambda f, ident: pltpu.make_async_remote_copy(
                src_ref=qsrc.at[c, f], dst_ref=qdst.at[me, c], send_sem=bulk_ss.at[g], recv_sem=bulk_rs.at[g],
                device_id=ident, device_id_type=MESH).start())
            return carry

        lax.fori_loop(c0, c0 + n, one, 0)

    def wait_bulk(g):
        c0, n = CHUNKS[g]
        ref = qdst.at[:, pl.ds(c0, n)]
        pltpu.make_async_copy(ref, ref, bulk_rs.at[g]).wait()

    w_copy.wait()
    my_base = (me * vloc).astype(F32)
    lane2 = lax.broadcasted_iota(jnp.int32, (LANES, vloc), 1).astype(F32)

    def matmul(t, carry):
        @pl.when(t + NBUF - 1 < npos * per_pos)
        def _():
            h_copy(t + NBUF - 1).start()

        h_copy(t).wait()
        i, r = t // per_pos, t % per_pos
        zb[...] = jnp.dot(hbuf[t % NBUF], wbuf[...], preferred_element_type=F32) * INV_TEMP
        for half in range(ROWS // LANES):
            blk = r * (ROWS // LANES) + half
            zz = zb[half * LANES:(half + 1) * LANES, :]
            m = jnp.max(zz, axis=1, keepdims=True)
            s = jnp.sum(jnp.exp(zz - m), axis=1, keepdims=True)
            ii = jnp.minimum(i, ndraft - 1)
            xblk = x_ref[:, pl.ds(pl.multiple_of(blk * LANES, LANES), LANES)].astype(F32)
            xrow = jnp.sum(jnp.where(sub4 == ii, xblk, 0.0), axis=0, keepdims=True) - my_base
            pick = jnp.sum(jnp.where(lane2 == to_col(xrow), zz, 0.0), axis=1, keepdims=True)
            qrow = jnp.sum(jnp.where((sub4 == ii) & (blk == me // 16), qp, 0.0), axis=0, keepdims=True)
            tile = jnp.where(sub4 == 0, to_row(m), jnp.where(sub4 == 1, to_row(s), jnp.where(
                sub4 == 2, to_row(pick), qrow)))
            st_send[blk * npos + i] = tile

            @pl.when(i < ndraft)
            def _():
                for lt in range(vloc // LANES):
                    zr[pl.ds(blk * LANES * 8 + lt * 4 + i, LANES, stride=8), :] = zz[:, lt * LANES:(lt + 1) * LANES]

            @pl.when(i == ndraft)
            def _():
                z4[pl.ds(pl.multiple_of(blk * LANES, LANES), LANES), :] = zz
        return carry

    lax.fori_loop(0, EARLY, matmul, 0)
    pl.semaphore_wait(barrier, nd - 1)
    send_bulk(0)
    lax.fori_loop(EARLY, npos * per_pos, matmul, 0)

    def owner(u):
        return u * 3

    is_owner = (me % 3 == 0) & (me < nunit * 3)
    my_unit = me // 3

    def send_stats(u, carry):
        f = owner(u)

        @pl.when(f != me)
        def _():
            pltpu.make_async_remote_copy(src_ref=st_send.at[u], dst_ref=st_recv.at[me], send_sem=st_ss, recv_sem=st_rs,
                                         device_id=dev(f), device_id_type=MESH).start()
        return carry

    lax.fori_loop(0, nunit, send_stats, 0)
    send_bulk(1)

    @pl.when(is_owner)
    def _():
        pltpu.make_async_copy(st_send.at[my_unit], st_recv.at[me], st_rs).start()
        pltpu.make_async_copy(st_recv, st_recv, st_rs).wait()
        mx = lax.fori_loop(0, nd, lambda s, m: jnp.maximum(m, st_recv[s]), st_recv[0])[0:1]

        def add(s, carry):
            t = st_recv[s]
            es, zp, qq = carry
            return es + jnp.exp(t[0:1] - mx) * t[1:2], zp + t[2:3], qq + t[3:4]

        zero = jnp.zeros((1, LANES), F32)
        es, zp, qq = lax.fori_loop(0, nd, add, (zero, zero, zero))
        accept = jnp.minimum(1.0, jnp.exp(zp - mx) / es / qq)
        ag_send[...] = jnp.where(sub4 == 0, mx, jnp.where(sub4 == 1, 1.0 / es, accept))
        pltpu.make_async_copy(ag_send, ag_recv.at[my_unit], ag_rs).start()
        each_peer(lambda f, ident: pltpu.make_async_remote_copy(
            src_ref=ag_send, dst_ref=ag_recv.at[my_unit], send_sem=ag_ss, recv_sem=ag_rs, device_id=ident,
            device_id_type=MESH).start(), far=True)

    for g in range(2, len(CHUNKS)):
        send_bulk(g)

    pltpu.make_async_copy(ag_recv, ag_recv, ag_rs).wait()

    def stat_rows(blk, k):
        return jnp.concatenate([ag_recv[blk * npos + i, k:k + 1, :] for i in range(ndraft)], axis=0)

    def probs(c0, n):
        def body(blk, carry):
            m8, r8 = twice(stat_rows(blk, 0)), twice(stat_rows(blk, 1))
            for j in range(LANES):
                if c0 <= j % per_src < c0 + n:
                    at = pl.ds(pl.multiple_of((blk * LANES + j) * 8, 8), 8)
                    zr[at, :] = jnp.exp(zr[at, :] - m8[:, j:j + 1]) * r8[:, j:j + 1]
            return carry
        lax.fori_loop(0, nblk, body, 0)

    def verdicts(blk, carry):
        a4 = stat_rows(blk, 2)
        cols = pl.ds(pl.multiple_of(blk * LANES, LANES), LANES)
        acc_ref[:, cols] = a4
        run, tot = a4[0:1], a4[0:1]
        for i in range(1, ndraft):
            run = run * a4[i:i + 1]
            tot = tot + run
        exp_ref[:, cols] = tot
        u4 = blk * npos + ndraft
        z4[cols, :] = jnp.exp(z4[cols, :] - to_col(ag_recv[u4, 0:1, :])) * to_col(ag_recv[u4, 1:2, :])
        return carry

    def excess(g):
        c0, n = CHUNKS[g]

        def body(s, accs):
            new = []
            for c in range(n):
                at = pl.ds(pl.multiple_of((s * per_src + c0 + c) * 8, 8), 8)
                e = jnp.maximum(zr[at, :] - qdst[s, c0 + c], 0.0)
                zr[at, :] = e
                new.append(jnp.where(lane == s, jnp.sum(e, axis=1, keepdims=True), accs[c]))
            return tuple(new)

        accs = lax.fori_loop(0, nd, body, tuple(jnp.zeros((8, LANES), F32) for _ in range(n)), unroll=4)
        for c in range(n):
            part = accs[c][:4] + accs[c][4:]
            zs_send[0, (c0 + c) // 2, ((c0 + c) % 2) * 4:((c0 + c) % 2) * 4 + 4] = part

    half = CHUNKS[2][0]
    probs(0, half)
    for g in range(2):
        wait_bulk(g)
        excess(g)
    probs(half, per_src - half)
    lax.fori_loop(0, nblk, verdicts, 0)
    for g in range(2, len(CHUNKS)):
        wait_bulk(g)
        excess(g)

    axes = [[{"tpa": cores[1], "tpb": me_b}],
            [{"tpa": me_a, "tpb": me_b - px + xs[k]} for k in (2, 1, 3)],
            [{"tpa": me_a, "tpb": me_b - py * 4 + ys[k]} for k in (2, 1, 3)],
            [{"tpa": me_a, "tpb": me_b - pz * 16 + ((pz + k) % 4) * 16} for k in (2, 1, 3)]]
    first = 0
    for t, group in enumerate(axes):
        for k, ident in enumerate(group):
            pltpu.make_async_remote_copy(src_ref=zs_send.at[t], dst_ref=zs_recv.at[first + k], send_sem=zs_ss.at[t],
                                         recv_sem=zs_rs.at[t], device_id=ident, device_id_type=MESH).start()
        ref = zs_recv.at[pl.ds(first, len(group))]
        pltpu.make_async_copy(ref, ref, zs_rs.at[t]).wait()
        total = zs_send[t]
        for k in range(len(group)):
            total = total + zs_recv[first + k]
        if t + 1 < len(axes):
            zs_send[t + 1] = total
        else:
            rz_ref[...] = 1.0 / total
        first += len(group)

    def drain(ref, sem):
        pltpu.make_async_copy(ref, ref, sem).wait()

    for g, (c0, n) in enumerate(CHUNKS):
        drain(qsrc.at[pl.ds(c0, n), pl.ds(0, nd - 1)], bulk_ss.at[g])

    @pl.when(is_owner)
    def _():
        drain(st_send.at[pl.ds(0, nunit - 1)], st_ss)
        drain(st_recv.at[pl.ds(0, nd - 1)], ag_ss)

    @pl.when(jnp.logical_not(is_owner))
    def _():
        drain(st_send, st_ss)

    for t, group in enumerate(axes):
        drain(zs_recv.at[pl.ds(0, len(group))], zs_ss.at[t])


def write_out(acc_ref, exp_ref, num_ref, bon_ref, rz_ref, acc_out, exp_out, res_out, bon_out, res, sem):
    nd, per_src = num_ref.shape[:2]
    small = [pltpu.make_async_copy(a, b, sem.at[k]) for k, (a, b) in enumerate(
        ((acc_ref, acc_out), (exp_ref, exp_out), (bon_ref, bon_out)))]
    for c in small:
        c.start()

    def put(c):
        return pltpu.make_async_copy(res.at[:, c], res_out.at[:, c], sem.at[3 + c])

    for c in range(per_src):
        tile = rz_ref[c // 2, (c % 2) * 4:(c % 2) * 4 + 4]
        r8 = jnp.concatenate([tile, tile], axis=0)
        for s in range(nd):
            res[s, c] = num_ref[s, c] * r8[:, s:s + 1]
        put(c).start()
    for c in range(per_src):
        put(c).wait()
    for c in small:
        c.wait()


def solution(mesh):
    na, nb = mesh.shape["tpa"], mesh.shape["tpb"]
    nd = na * nb

    def local_step(hidden, w_head, q_draft, x_draft):
        nseq, npos, dm = hidden.shape
        ndraft = npos - 1
        vloc = w_head.shape[1]
        per_src = q_draft.shape[0]
        nt = vloc // LANES
        h5 = jnp.transpose(hidden, (1, 0, 2))
        q4 = q_draft.reshape(per_src, ndraft, nd, nt, LANES).transpose(0, 2, 3, 1, 4).reshape(per_src, nd, nt * ndraft,
                                                                                             LANES)
        xt = x_draft.T
        nunit = (nseq // LANES) * npos
        hbm = pl.BlockSpec(memory_space=pltpu.HBM)
        vmem = pl.BlockSpec(memory_space=pltpu.VMEM)
        dma, vm = pltpu.SemaphoreType.DMA, pltpu.VMEM
        outs = pl.pallas_call(
            functools.partial(kernel, (na, nb)),
            out_shape=[
                jax.ShapeDtypeStruct((ndraft, nseq), F32),
                jax.ShapeDtypeStruct((1, nseq), F32),
                jax.ShapeDtypeStruct((nseq * nt * ndraft, LANES), F32),
                jax.ShapeDtypeStruct((nseq, vloc), F32),
                jax.ShapeDtypeStruct((per_src // 2, 8, LANES), F32),
            ],
            in_specs=[hbm] * 4,
            out_specs=[vmem] * 5,
            scratch_shapes=[
                vm((NBUF, ROWS, dm), jnp.bfloat16),
                vm((dm, vloc), jnp.bfloat16),
                vm((ndraft, nseq), jnp.int32),
                vm((per_src, nd, 8, LANES), F32),
                vm((nd, per_src, 8, LANES), F32),
                vm((ROWS, vloc), F32),
                vm((nunit, 4, LANES), F32),
                vm((nd, 4, LANES), F32),
                vm((4, LANES), F32),
                vm((nunit, 4, LANES), F32),
                vm((4, per_src // 2, 8, LANES), F32),
                vm((10, per_src // 2, 8, LANES), F32),
                dma((NBUF,)), dma, dma, dma, dma((len(CHUNKS),)), dma((len(CHUNKS),)), dma, dma, dma, dma, dma((4,)),
                dma((4,)),
            ],
            compiler_params=pltpu.CompilerParams(collective_id=0, has_side_effects=True,
                                                 vmem_limit_bytes=46 * 1024 * 1024),
            name="verify",
        )(*[pltpu.with_memory_space_constraint(a, pltpu.HBM) for a in (h5, w_head, q4, xt)])
        acc, exp, num, bonus, rz = outs
        num = num.reshape(nd, per_src, nt * ndraft, LANES)
        outs = (acc, exp, num, bonus)
        acc, exp, res, bonus = pl.pallas_call(
            write_out,
            out_shape=[jax.ShapeDtypeStruct(o.shape, o.dtype) for o in outs],
            in_specs=[vmem] * 5,
            out_specs=[hbm] * 4,
            scratch_shapes=[vm(num.shape, F32), dma((3 + per_src,))],
            compiler_params=pltpu.CompilerParams(vmem_limit_bytes=8 * 1024 * 1024),
            name="write_out",
        )(*outs, rz)
        residual = res.reshape(nseq, nt, ndraft, LANES).transpose(0, 2, 1, 3).reshape(nseq, ndraft, vloc)
        return acc.T, exp.reshape(nseq), residual, bonus

    return jax.shard_map(
        local_step, mesh=mesh,
        in_specs=(P("dp", None, None), P(None, VOCAB_AXES), P(("dp",) + VOCAB_AXES, None, None), P("dp", None)),
        out_specs=(P("dp", None), P("dp"), P("dp", None, VOCAB_AXES), P("dp", VOCAB_AXES)),
        check_vma=False)
```

```python
import functools

import jax
import jax.numpy as jnp
from jax import lax
from jax.experimental import pallas as pl
from jax.experimental.pallas import tpu as pltpu
from jax.sharding import PartitionSpec as P

INV_TEMP = 1.25
VOCAB_AXES = ("tpa", "tpb")
MESH = pl.DeviceIdType.MESH
F32 = jnp.float32
LANES = 128
CHUNKS = ((0, 3), (3, 2), (5, 1), (6, 1), (7, 1))
ROWS = 256
NBUF = 3
EARLY = 3


def kernel(dims, h_ref, w_ref, q_ref, xin_ref, acc_ref, exp_ref, zr, z4, rz_ref,
           hbuf, wbuf, x_ref, qsrc, qdst, zb, st_send, st_recv, ag_send, ag_recv, zs_send, zs_recv, h_sem, w_sem, q_sem,
           x_sem, bulk_ss, bulk_rs, st_ss, st_rs, ag_ss, ag_rs, zs_ss, zs_rs):
    na, nb = dims
    nd = na * nb
    me_a, me_b = lax.axis_index("tpa"), lax.axis_index("tpb")
    me = me_a * nb + me_b
    npos = h_ref.shape[0]
    ndraft = npos - 1
    nseq = h_ref.shape[1]
    nblk = nseq // LANES
    nunit = nblk * npos
    per_src = nseq // nd
    vloc = w_ref.shape[1]

    def dev(f):
        return {"tpa": f // nb, "tpb": f % nb}

    px, py, pz = me_b % 4, (me_b // 4) % 4, me_b // 16
    xs = [(px + k) % 4 for k in range(4)]
    ys = [((py + k) % 4) * 4 for k in range(4)]
    cores = [me_a, (me_a + 1) % na]

    def each_peer(fn, far=False):
        first = 2 if far else 0

        def plane(kz, carry):
            zz = pz + kz + first
            zz = jnp.where(zz >= 4, zz - 4, zz)
            base = jnp.where(zz >= 4, zz - 4, zz) * 16
            for ky in (2, 1, 3, 0) if far else range(4):
                for kx in (2, 1, 3, 0) if far else (1, 3, 2, 0):
                    for ka in range(na):
                        b = base + ys[ky] + xs[kx]
                        f = cores[ka] * nb + b
                        ident = {"tpa": cores[ka], "tpb": b}
                        if ka == kx == ky == 0:
                            @pl.when(kz != (4 - first) % 4)
                            def _():
                                fn(f, ident)
                        else:
                            fn(f, ident)
            return carry
        lax.fori_loop(0, 4, plane, 0)

    lane = lax.broadcasted_iota(jnp.int32, (8, LANES), 1)
    sub = lax.broadcasted_iota(jnp.int32, (8, LANES), 0)
    sub4 = lax.broadcasted_iota(jnp.int32, (4, LANES), 0)
    lane_f = lane.astype(F32)
    eye = (lax.broadcasted_iota(jnp.int32, (LANES, LANES), 0) == lax.broadcasted_iota(jnp.int32, (LANES, LANES), 1))

    def to_col(row):
        return jnp.sum(jnp.where(eye, jnp.broadcast_to(row, (LANES, LANES)), 0.0), axis=1, keepdims=True)

    def to_row(col):
        return jnp.sum(jnp.where(eye, jnp.broadcast_to(col, (LANES, LANES)), 0.0), axis=0, keepdims=True)

    def twice(t):
        return jnp.concatenate([t, t], axis=0)

    q_copy = pltpu.make_async_copy(q_ref, qsrc, q_sem)
    q_copy.start()
    w_copy = pltpu.make_async_copy(w_ref, wbuf, w_sem)
    w_copy.start()
    per_pos = nseq // ROWS

    def h_copy(t):
        return pltpu.make_async_copy(h_ref.at[t // per_pos, pl.ds((t % per_pos) * ROWS, ROWS)], hbuf.at[t % NBUF],
                                     h_sem.at[t % NBUF])

    x_copy = pltpu.make_async_copy(xin_ref, x_ref, x_sem)
    x_copy.start()
    for t in range(NBUF - 1):
        h_copy(t).start()

    barrier = pltpu.get_barrier_semaphore()
    each_peer(lambda f, ident: pl.semaphore_signal(barrier, inc=1, device_id=ident, device_id_type=MESH), far=True)
    q_copy.wait()

    def local_bulk(g):
        c0, n = CHUNKS[g]
        return pltpu.make_async_copy(qsrc.at[pl.ds(c0, n), me], qdst.at[me, pl.ds(c0, n)], bulk_rs.at[g])

    for g in range(len(CHUNKS)):
        local_bulk(g).start()
    x_copy.wait()
    xb = x_ref[:, pl.ds(pl.multiple_of((me // 16) * LANES, LANES), LANES)].astype(F32)
    targets = []
    for c in range(per_src):
        j = (me % 16) * per_src + c
        col = jnp.sum(jnp.where(lane[:4] == j, xb, 0.0), axis=1, keepdims=True)
        targets.append(twice(jnp.broadcast_to(col, (4, LANES))) - jnp.where(sub >= 4, F32(LANES), F32(0)) - lane_f)

    def pick_q(d, accs):
        base = (d * vloc).astype(F32)
        return tuple(a + jnp.where(t == base, qsrc[c, d], 0.0) for c, (a, t) in enumerate(zip(accs, targets)))

    accs = lax.fori_loop(0, nd, pick_q, tuple(jnp.zeros((8, LANES), F32) for _ in range(per_src)),
                         unroll=8)
    qp = jnp.zeros((4, LANES), F32)
    for c in range(per_src):
        col = jnp.sum(accs[c], axis=1, keepdims=True)
        qp = jnp.where(lane[:4] == (me % 16) * per_src + c, col[:4] + col[4:], qp)


    def send_bulk(g):
        c0, n = CHUNKS[g]

        def one(c, carry):
            each_peer(lambda f, ident: pltpu.make_async_remote_copy(
                src_ref=qsrc.at[c, f], dst_ref=qdst.at[me, c], send_sem=bulk_ss.at[g], recv_sem=bulk_rs.at[g],
                device_id=ident, device_id_type=MESH).start())
            return carry

        lax.fori_loop(c0, c0 + n, one, 0)

    def wait_bulk(g):
        c0, n = CHUNKS[g]
        ref = qdst.at[:, pl.ds(c0, n)]
        pltpu.make_async_copy(ref, ref, bulk_rs.at[g]).wait()

    w_copy.wait()
    my_base = (me * vloc).astype(F32)
    lane2 = lax.broadcasted_iota(jnp.int32, (LANES, vloc), 1).astype(F32)

    def matmul(t, carry):
        @pl.when(t + NBUF - 1 < npos * per_pos)
        def _():
            h_copy(t + NBUF - 1).start()

        h_copy(t).wait()
        i, r = t // per_pos, t % per_pos
        zb[...] = jnp.dot(hbuf[t % NBUF], wbuf[...], preferred_element_type=F32) * INV_TEMP
        for half in range(ROWS // LANES):
            blk = r * (ROWS // LANES) + half
            zz = zb[half * LANES:(half + 1) * LANES, :]
            m = jnp.max(zz, axis=1, keepdims=True)
            s = jnp.sum(jnp.exp(zz - m), axis=1, keepdims=True)
            ii = jnp.minimum(i, ndraft - 1)
            xblk = x_ref[:, pl.ds(pl.multiple_of(blk * LANES, LANES), LANES)].astype(F32)
            xrow = jnp.sum(jnp.where(sub4 == ii, xblk, 0.0), axis=0, keepdims=True) - my_base
            pick = jnp.sum(jnp.where(lane2 == to_col(xrow), zz, 0.0), axis=1, keepdims=True)
            qrow = jnp.sum(jnp.where((sub4 == ii) & (blk == me // 16), qp, 0.0), axis=0, keepdims=True)
            tile = jnp.where(sub4 == 0, to_row(m), jnp.where(sub4 == 1, to_row(s), jnp.where(
                sub4 == 2, to_row(pick), qrow)))
            st_send[blk * npos + i] = tile

            @pl.when(i < ndraft)
            def _():
                for lt in range(vloc // LANES):
                    zr[pl.ds(blk * LANES * 8 + lt * 4 + i, LANES, stride=8), :] = zz[:, lt * LANES:(lt + 1) * LANES]

            @pl.when(i == ndraft)
            def _():
                z4[pl.ds(pl.multiple_of(blk * LANES, LANES), LANES), :] = zz
        return carry

    lax.fori_loop(0, EARLY, matmul, 0)
    pl.semaphore_wait(barrier, nd - 1)
    send_bulk(0)
    lax.fori_loop(EARLY, npos * per_pos, matmul, 0)

    def owner(u):
        return u * 3

    is_owner = (me % 3 == 0) & (me < nunit * 3)
    my_unit = me // 3

    def send_stats(u, carry):
        f = owner(u)

        @pl.when(f != me)
        def _():
            pltpu.make_async_remote_copy(src_ref=st_send.at[u], dst_ref=st_recv.at[me], send_sem=st_ss, recv_sem=st_rs,
                                         device_id=dev(f), device_id_type=MESH).start()
        return carry

    lax.fori_loop(0, nunit, send_stats, 0)
    send_bulk(1)

    @pl.when(is_owner)
    def _():
        pltpu.make_async_copy(st_send.at[my_unit], st_recv.at[me], st_rs).start()
        pltpu.make_async_copy(st_recv, st_recv, st_rs).wait()
        mx = lax.fori_loop(0, nd, lambda s, m: jnp.maximum(m, st_recv[s]), st_recv[0], unroll=8)[0:1]

        def add(s, carry):
            t = st_recv[s]
            es, zp, qq = carry
            return es + jnp.exp(t[0:1] - mx) * t[1:2], zp + t[2:3], qq + t[3:4]

        zero = jnp.zeros((1, LANES), F32)
        es, zp, qq = lax.fori_loop(0, nd, add, (zero, zero, zero), unroll=8)
        accept = jnp.minimum(1.0, jnp.exp(zp - mx) / es / qq)
        ag_send[...] = jnp.where(sub4 == 0, mx, jnp.where(sub4 == 1, 1.0 / es, accept))
        pltpu.make_async_copy(ag_send, ag_recv.at[my_unit], ag_rs).start()
        each_peer(lambda f, ident: pltpu.make_async_remote_copy(
            src_ref=ag_send, dst_ref=ag_recv.at[my_unit], send_sem=ag_ss, recv_sem=ag_rs, device_id=ident,
            device_id_type=MESH).start(), far=True)

    for g in range(2, len(CHUNKS)):
        send_bulk(g)

    pltpu.make_async_copy(ag_recv, ag_recv, ag_rs).wait()

    def stat_rows(blk, k):
        return jnp.concatenate([ag_recv[blk * npos + i, k:k + 1, :] for i in range(ndraft)], axis=0)

    def probs(c0, n):
        def body(blk, carry):
            m8, r8 = twice(stat_rows(blk, 0)), twice(stat_rows(blk, 1))
            for j in range(LANES):
                if c0 <= j % per_src < c0 + n:
                    at = pl.ds(pl.multiple_of((blk * LANES + j) * 8, 8), 8)
                    zr[at, :] = jnp.exp(zr[at, :] - m8[:, j:j + 1]) * r8[:, j:j + 1]
            return carry
        lax.fori_loop(0, nblk, body, 0)

    def verdicts(blk, carry):
        a4 = stat_rows(blk, 2)
        cols = pl.ds(pl.multiple_of(blk * LANES, LANES), LANES)
        acc_ref[:, cols] = a4
        run, tot = a4[0:1], a4[0:1]
        for i in range(1, ndraft):
            run = run * a4[i:i + 1]
            tot = tot + run
        exp_ref[:, cols] = tot
        u4 = blk * npos + ndraft
        z4[cols, :] = jnp.exp(z4[cols, :] - to_col(ag_recv[u4, 0:1, :])) * to_col(ag_recv[u4, 1:2, :])
        return carry

    def excess(g):
        c0, n = CHUNKS[g]

        def body(s, accs):
            new = []
            for c in range(n):
                at = pl.ds(pl.multiple_of((s * per_src + c0 + c) * 8, 8), 8)
                e = jnp.maximum(zr[at, :] - qdst[s, c0 + c], 0.0)
                zr[at, :] = e
                new.append(jnp.where(lane == s, jnp.sum(e, axis=1, keepdims=True), accs[c]))
            return tuple(new)

        accs = lax.fori_loop(0, nd, body, tuple(jnp.zeros((8, LANES), F32) for _ in range(n)), unroll=4)
        for c in range(n):
            part = accs[c][:4] + accs[c][4:]
            zs_send[0, (c0 + c) // 2, ((c0 + c) % 2) * 4:((c0 + c) % 2) * 4 + 4] = part

    half = CHUNKS[2][0]
    probs(0, half)
    for g in range(2):
        wait_bulk(g)
        excess(g)
    probs(half, per_src - half)
    for g in range(2, len(CHUNKS)):
        wait_bulk(g)
        excess(g)

    axes = [[{"tpa": cores[a], "tpb": me_b - px + xs[k]} for k in (2, 1, 3, 0) for a in range(na) if (k, a) != (0, 0)],
            [{"tpa": me_a, "tpb": me_b - py * 4 + ys[k]} for k in (2, 1, 3)],
            [{"tpa": me_a, "tpb": me_b - pz * 16 + ((pz + k) % 4) * 16} for k in (2, 1, 3)]]
    first = 0
    for t, group in enumerate(axes):
        for k, ident in enumerate(group):
            pltpu.make_async_remote_copy(src_ref=zs_send.at[t], dst_ref=zs_recv.at[first + k], send_sem=zs_ss.at[t],
                                         recv_sem=zs_rs.at[t], device_id=ident, device_id_type=MESH).start()
        if t == 0:
            lax.fori_loop(0, nblk, verdicts, 0)
        ref = zs_recv.at[pl.ds(first, len(group))]
        pltpu.make_async_copy(ref, ref, zs_rs.at[t]).wait()
        total = zs_send[t]
        for k in range(len(group)):
            total = total + zs_recv[first + k]
        if t + 1 < len(axes):
            zs_send[t + 1] = total
        else:
            rz_ref[...] = 1.0 / total
        first += len(group)

    def drain(ref, sem):
        pltpu.make_async_copy(ref, ref, sem).wait()

    for g, (c0, n) in enumerate(CHUNKS):
        drain(qsrc.at[pl.ds(c0, n), pl.ds(0, nd - 1)], bulk_ss.at[g])

    @pl.when(is_owner)
    def _():
        drain(st_send.at[pl.ds(0, nunit - 1)], st_ss)
        drain(st_recv.at[pl.ds(0, nd - 1)], ag_ss)

    @pl.when(jnp.logical_not(is_owner))
    def _():
        drain(st_send, st_ss)

    for t, group in enumerate(axes):
        drain(zs_recv.at[pl.ds(0, len(group))], zs_ss.at[t])


def write_out(acc_ref, exp_ref, num_ref, bon_ref, rz_ref, acc_out, exp_out, res_out, bon_out, res, sem):
    nd, per_src = num_ref.shape[:2]
    small = [pltpu.make_async_copy(a, b, sem.at[k]) for k, (a, b) in enumerate(
        ((acc_ref, acc_out), (exp_ref, exp_out), (bon_ref, bon_out)))]
    for c in small:
        c.start()

    def put(c):
        return pltpu.make_async_copy(res.at[:, c], res_out.at[:, c], sem.at[3 + c])

    for c in range(per_src):
        tile = rz_ref[c // 2, (c % 2) * 4:(c % 2) * 4 + 4]
        r8 = jnp.concatenate([tile, tile], axis=0)
        for s in range(nd):
            res[s, c] = num_ref[s, c] * r8[:, s:s + 1]
        put(c).start()
    for c in range(per_src):
        put(c).wait()
    for c in small:
        c.wait()


def solution(mesh):
    na, nb = mesh.shape["tpa"], mesh.shape["tpb"]
    nd = na * nb

    def local_step(hidden, w_head, q_draft, x_draft):
        nseq, npos, dm = hidden.shape
        ndraft = npos - 1
        vloc = w_head.shape[1]
        per_src = q_draft.shape[0]
        nt = vloc // LANES
        h5 = jnp.transpose(hidden, (1, 0, 2))
        q4 = q_draft.reshape(per_src, ndraft, nd, nt, LANES).transpose(0, 2, 3, 1, 4).reshape(per_src, nd, nt * ndraft,
                                                                                             LANES)
        xt = x_draft.T
        nunit = (nseq // LANES) * npos
        hbm = pl.BlockSpec(memory_space=pltpu.HBM)
        vmem = pl.BlockSpec(memory_space=pltpu.VMEM)
        dma, vm = pltpu.SemaphoreType.DMA, pltpu.VMEM
        outs = pl.pallas_call(
            functools.partial(kernel, (na, nb)),
            out_shape=[
                jax.ShapeDtypeStruct((ndraft, nseq), F32),
                jax.ShapeDtypeStruct((1, nseq), F32),
                jax.ShapeDtypeStruct((nseq * nt * ndraft, LANES), F32),
                jax.ShapeDtypeStruct((nseq, vloc), F32),
                jax.ShapeDtypeStruct((per_src // 2, 8, LANES), F32),
            ],
            in_specs=[hbm] * 4,
            out_specs=[vmem] * 5,
            scratch_shapes=[
                vm((NBUF, ROWS, dm), jnp.bfloat16),
                vm((dm, vloc), jnp.bfloat16),
                vm((ndraft, nseq), jnp.int32),
                vm((per_src, nd, 8, LANES), F32),
                vm((nd, per_src, 8, LANES), F32),
                vm((ROWS, vloc), F32),
                vm((nunit, 4, LANES), F32),
                vm((nd, 4, LANES), F32),
                vm((4, LANES), F32),
                vm((nunit, 4, LANES), F32),
                vm((3, per_src // 2, 8, LANES), F32),
                vm((13, per_src // 2, 8, LANES), F32),
                dma((NBUF,)), dma, dma, dma, dma((len(CHUNKS),)), dma((len(CHUNKS),)), dma, dma, dma, dma, dma((3,)),
                dma((3,)),
            ],
            compiler_params=pltpu.CompilerParams(collective_id=0, has_side_effects=True,
                                                 vmem_limit_bytes=46 * 1024 * 1024),
            name="verify",
        )(*[pltpu.with_memory_space_constraint(a, pltpu.HBM) for a in (h5, w_head, q4, xt)])
        acc, exp, num, bonus, rz = outs
        num = num.reshape(nd, per_src, nt * ndraft, LANES)
        outs = (acc, exp, num, bonus)
        acc, exp, res, bonus = pl.pallas_call(
            write_out,
            out_shape=[jax.ShapeDtypeStruct(o.shape, o.dtype) for o in outs],
            in_specs=[vmem] * 5,
            out_specs=[hbm] * 4,
            scratch_shapes=[vm(num.shape, F32), dma((3 + per_src,))],
            compiler_params=pltpu.CompilerParams(vmem_limit_bytes=8 * 1024 * 1024),
            name="write_out",
        )(*outs, rz)
        residual = res.reshape(nseq, nt, ndraft, LANES).transpose(0, 2, 1, 3).reshape(nseq, ndraft, vloc)
        return acc.T, exp.reshape(nseq), residual, bonus

    return jax.shard_map(
        local_step, mesh=mesh,
        in_specs=(P("dp", None, None), P(None, VOCAB_AXES), P(("dp",) + VOCAB_AXES, None, None), P("dp", None)),
        out_specs=(P("dp", None), P("dp"), P("dp", None, VOCAB_AXES), P("dp", VOCAB_AXES)),
        check_vma=False)
```

```python
import functools

import jax
import jax.numpy as jnp
from jax import lax
from jax.experimental import pallas as pl
from jax.experimental.pallas import tpu as pltpu
from jax.sharding import PartitionSpec as P

INV_TEMP = 1.25
VOCAB_AXES = ("tpa", "tpb")
MESH = pl.DeviceIdType.MESH
F32 = jnp.float32
LANES = 128
CHUNKS = ((0, 3), (3, 1), (4, 1), (5, 2), (7, 1))
ROWS = 256
NBUF = 3
EARLY = 3


def kernel(dims, h_ref, w_ref, q_ref, xin_ref, acc_ref, exp_ref, zr, z4, rz_ref,
           hbuf, wbuf, x_ref, qsrc, qdst, zb, st_send, st_recv, ag_send, ag_recv, zs_send, zs_recv, h_sem, w_sem, q_sem,
           x_sem, bulk_ss, bulk_rs, st_ss, st_rs, ag_ss, ag_rs, zs_ss, zs_rs):
    na, nb = dims
    nd = na * nb
    me_a, me_b = lax.axis_index("tpa"), lax.axis_index("tpb")
    me = me_a * nb + me_b
    npos = h_ref.shape[0]
    ndraft = npos - 1
    nseq = h_ref.shape[1]
    nblk = nseq // LANES
    nunit = nblk * npos
    per_src = nseq // nd
    vloc = w_ref.shape[1]

    def dev(f):
        return {"tpa": f // nb, "tpb": f % nb}

    px, py, pz = me_b % 4, (me_b // 4) % 4, me_b // 16
    xs = [(px + k) % 4 for k in range(4)]
    ys = [((py + k) % 4) * 4 for k in range(4)]
    cores = [me_a, (me_a + 1) % na]

    def each_peer(fn, far=False, own_core=False):
        first = 2 if far else 0

        def plane(kz, carry):
            zz = pz + kz + first
            zz = jnp.where(zz >= 4, zz - 4, zz)
            base = jnp.where(zz >= 4, zz - 4, zz) * 16
            for ky in (2, 1, 3, 0) if far else range(4):
                for kx in (2, 1, 3, 0) if far else (1, 3, 2, 0):
                    for ka in range(1 if own_core else na):
                        b = base + ys[ky] + xs[kx]
                        f = cores[ka] * nb + b
                        ident = {"tpa": cores[ka], "tpb": b}
                        if ka == kx == ky == 0:
                            @pl.when(kz != (4 - first) % 4)
                            def _():
                                fn(f, ident)
                        else:
                            fn(f, ident)
            return carry
        lax.fori_loop(0, 4, plane, 0)

    lane = lax.broadcasted_iota(jnp.int32, (8, LANES), 1)
    sub = lax.broadcasted_iota(jnp.int32, (8, LANES), 0)
    sub4 = lax.broadcasted_iota(jnp.int32, (4, LANES), 0)
    lane_f = lane.astype(F32)
    eye = (lax.broadcasted_iota(jnp.int32, (LANES, LANES), 0) == lax.broadcasted_iota(jnp.int32, (LANES, LANES), 1))

    def to_col(row):
        return jnp.sum(jnp.where(eye, jnp.broadcast_to(row, (LANES, LANES)), 0.0), axis=1, keepdims=True)

    def to_row(col):
        return jnp.sum(jnp.where(eye, jnp.broadcast_to(col, (LANES, LANES)), 0.0), axis=0, keepdims=True)

    def twice(t):
        return jnp.concatenate([t, t], axis=0)

    q_copy = pltpu.make_async_copy(q_ref, qsrc, q_sem)
    q_copy.start()
    w_copy = pltpu.make_async_copy(w_ref, wbuf, w_sem)
    w_copy.start()
    per_pos = nseq // ROWS

    def h_copy(t):
        return pltpu.make_async_copy(h_ref.at[t // per_pos, pl.ds((t % per_pos) * ROWS, ROWS)], hbuf.at[t % NBUF],
                                     h_sem.at[t % NBUF])

    x_copy = pltpu.make_async_copy(xin_ref, x_ref, x_sem)
    x_copy.start()
    for t in range(NBUF - 1):
        h_copy(t).start()

    barrier = pltpu.get_barrier_semaphore()
    each_peer(lambda f, ident: pl.semaphore_signal(barrier, inc=1, device_id=ident, device_id_type=MESH), far=True)
    q_copy.wait()

    def local_bulk(g):
        c0, n = CHUNKS[g]
        return pltpu.make_async_copy(qsrc.at[pl.ds(c0, n), me], qdst.at[me, pl.ds(c0, n)], bulk_rs.at[g])

    for g in range(len(CHUNKS)):
        local_bulk(g).start()
    x_copy.wait()
    xb = x_ref[:, pl.ds(pl.multiple_of((me // 16) * LANES, LANES), LANES)].astype(F32)
    targets = []
    for c in range(per_src):
        j = (me % 16) * per_src + c
        col = jnp.sum(jnp.where(lane[:4] == j, xb, 0.0), axis=1, keepdims=True)
        targets.append(twice(jnp.broadcast_to(col, (4, LANES))) - jnp.where(sub >= 4, F32(LANES), F32(0)) - lane_f)

    def pick_q(d, accs):
        base = (d * vloc).astype(F32)
        return tuple(a + jnp.where(t == base, qsrc[c, d], 0.0) for c, (a, t) in enumerate(zip(accs, targets)))

    accs = lax.fori_loop(0, nd, pick_q, tuple(jnp.zeros((8, LANES), F32) for _ in range(per_src)),
                         unroll=8)
    qp = jnp.zeros((4, LANES), F32)
    for c in range(per_src):
        col = jnp.sum(accs[c], axis=1, keepdims=True)
        qp = jnp.where(lane[:4] == (me % 16) * per_src + c, col[:4] + col[4:], qp)


    def send_bulk(g):
        c0, n = CHUNKS[g]

        def one(c, carry):
            each_peer(lambda f, ident: pltpu.make_async_remote_copy(
                src_ref=qsrc.at[c, f], dst_ref=qdst.at[me, c], send_sem=bulk_ss.at[g], recv_sem=bulk_rs.at[g],
                device_id=ident, device_id_type=MESH).start())
            return carry

        lax.fori_loop(c0, c0 + n, one, 0)

    def wait_bulk(g):
        c0, n = CHUNKS[g]
        ref = qdst.at[:, pl.ds(c0, n)]
        pltpu.make_async_copy(ref, ref, bulk_rs.at[g]).wait()

    w_copy.wait()
    my_base = (me * vloc).astype(F32)
    lane2 = lax.broadcasted_iota(jnp.int32, (LANES, vloc), 1).astype(F32)

    def matmul(t, carry):
        @pl.when(t + NBUF - 1 < npos * per_pos)
        def _():
            h_copy(t + NBUF - 1).start()

        h_copy(t).wait()
        i, r = t // per_pos, t % per_pos
        zb[...] = jnp.dot(hbuf[t % NBUF], wbuf[...], preferred_element_type=F32) * INV_TEMP
        for half in range(ROWS // LANES):
            blk = r * (ROWS // LANES) + half
            zz = zb[half * LANES:(half + 1) * LANES, :]
            m = jnp.max(zz, axis=1, keepdims=True)
            s = jnp.sum(jnp.exp(zz - m), axis=1, keepdims=True)
            ii = jnp.minimum(i, ndraft - 1)
            xblk = x_ref[:, pl.ds(pl.multiple_of(blk * LANES, LANES), LANES)].astype(F32)
            xrow = jnp.sum(jnp.where(sub4 == ii, xblk, 0.0), axis=0, keepdims=True) - my_base
            pick = jnp.sum(jnp.where(lane2 == to_col(xrow), zz, 0.0), axis=1, keepdims=True)
            qrow = jnp.sum(jnp.where((sub4 == ii) & (blk == me // 16), qp, 0.0), axis=0, keepdims=True)
            tile = jnp.where(sub4 == 0, to_row(m), jnp.where(sub4 == 1, to_row(s), jnp.where(
                sub4 == 2, to_row(pick), qrow)))
            st_send[blk * npos + i] = tile

            @pl.when(i < ndraft)
            def _():
                for lt in range(vloc // LANES):
                    zr[pl.ds(blk * LANES * 8 + lt * 4 + i, LANES, stride=8), :] = zz[:, lt * LANES:(lt + 1) * LANES]

            @pl.when(i == ndraft)
            def _():
                z4[pl.ds(pl.multiple_of(blk * LANES, LANES), LANES), :] = zz
        return carry

    lax.fori_loop(0, EARLY, matmul, 0)
    pl.semaphore_wait(barrier, nd - 1)
    send_bulk(0)
    lax.fori_loop(EARLY, npos * per_pos, matmul, 0)

    my_unit = (me_b * 43) % nb
    is_owner = my_unit < nunit

    def send_stats(u, carry):
        chip = (u * 3) % nb
        for a in range(na):
            @pl.when((chip != me_b) | (me_a != a))
            def _():
                pltpu.make_async_remote_copy(src_ref=st_send.at[u], dst_ref=st_recv.at[me], send_sem=st_ss,
                                             recv_sem=st_rs, device_id={"tpa": a, "tpb": chip},
                                             device_id_type=MESH).start()
        return carry

    lax.fori_loop(0, nunit, send_stats, 0)
    send_bulk(1)

    @pl.when(is_owner)
    def _():
        pltpu.make_async_copy(st_send.at[my_unit], st_recv.at[me], st_rs).start()
        pltpu.make_async_copy(st_recv, st_recv, st_rs).wait()
        mx = lax.fori_loop(0, nd, lambda s, m: jnp.maximum(m, st_recv[s]), st_recv[0], unroll=8)[0:1]

        def add(s, carry):
            t = st_recv[s]
            es, zp, qq = carry
            return es + jnp.exp(t[0:1] - mx) * t[1:2], zp + t[2:3], qq + t[3:4]

        zero = jnp.zeros((1, LANES), F32)
        es, zp, qq = lax.fori_loop(0, nd, add, (zero, zero, zero), unroll=8)
        accept = jnp.minimum(1.0, jnp.exp(zp - mx) / es / qq)
        ag_send[...] = jnp.where(sub4 == 0, mx, jnp.where(sub4 == 1, 1.0 / es, accept))
        pltpu.make_async_copy(ag_send, ag_recv.at[my_unit], ag_rs).start()
        each_peer(lambda f, ident: pltpu.make_async_remote_copy(
            src_ref=ag_send, dst_ref=ag_recv.at[my_unit], send_sem=ag_ss, recv_sem=ag_rs, device_id=ident,
            device_id_type=MESH).start(), far=True, own_core=True)

    send_bulk(2)

    pltpu.make_async_copy(ag_recv, ag_recv, ag_rs).wait()
    for g in range(3, len(CHUNKS)):
        send_bulk(g)

    def stat_rows(blk, k):
        return jnp.concatenate([ag_recv[blk * npos + i, k:k + 1, :] for i in range(ndraft)], axis=0)

    def probs(c0, n):
        def body(blk, carry):
            m8, r8 = twice(stat_rows(blk, 0)), twice(stat_rows(blk, 1))
            for j in range(LANES):
                if c0 <= j % per_src < c0 + n:
                    at = pl.ds(pl.multiple_of((blk * LANES + j) * 8, 8), 8)
                    zr[at, :] = jnp.exp(zr[at, :] - m8[:, j:j + 1]) * r8[:, j:j + 1]
            return carry
        lax.fori_loop(0, nblk, body, 0)

    def verdicts(blk, carry):
        a4 = stat_rows(blk, 2)
        cols = pl.ds(pl.multiple_of(blk * LANES, LANES), LANES)
        acc_ref[:, cols] = a4
        run, tot = a4[0:1], a4[0:1]
        for i in range(1, ndraft):
            run = run * a4[i:i + 1]
            tot = tot + run
        exp_ref[:, cols] = tot
        u4 = blk * npos + ndraft
        z4[cols, :] = jnp.exp(z4[cols, :] - to_col(ag_recv[u4, 0:1, :])) * to_col(ag_recv[u4, 1:2, :])
        return carry

    def excess(g):
        c0, n = CHUNKS[g]

        def body(s, accs):
            new = []
            for c in range(n):
                at = pl.ds(pl.multiple_of((s * per_src + c0 + c) * 8, 8), 8)
                e = jnp.maximum(zr[at, :] - qdst[s, c0 + c], 0.0)
                zr[at, :] = e
                new.append(jnp.where(lane == s, jnp.sum(e, axis=1, keepdims=True), accs[c]))
            return tuple(new)

        accs = lax.fori_loop(0, nd, body, tuple(jnp.zeros((8, LANES), F32) for _ in range(n)), unroll=4)
        for c in range(n):
            part = accs[c][:4] + accs[c][4:]
            zs_send[0, (c0 + c) // 2, ((c0 + c) % 2) * 4:((c0 + c) % 2) * 4 + 4] = part

    half = CHUNKS[2][0]
    probs(0, half)
    for g in range(2):
        wait_bulk(g)
        excess(g)
    probs(half, per_src - half)
    for g in range(2, len(CHUNKS)):
        wait_bulk(g)
        excess(g)

    axes = [[{"tpa": cores[a], "tpb": me_b - px + xs[k]} for k in (2, 1, 3, 0) for a in range(na) if (k, a) != (0, 0)],
            [{"tpa": me_a, "tpb": me_b - py * 4 + ys[k]} for k in (2, 1, 3)],
            [{"tpa": me_a, "tpb": me_b - pz * 16 + ((pz + k) % 4) * 16} for k in (2, 1, 3)]]
    first = 0
    for t, group in enumerate(axes):
        for k, ident in enumerate(group):
            pltpu.make_async_remote_copy(src_ref=zs_send.at[t], dst_ref=zs_recv.at[first + k], send_sem=zs_ss.at[t],
                                         recv_sem=zs_rs.at[t], device_id=ident, device_id_type=MESH).start()
        if t == 0:
            lax.fori_loop(0, nblk, verdicts, 0)
        ref = zs_recv.at[pl.ds(first, len(group))]
        pltpu.make_async_copy(ref, ref, zs_rs.at[t]).wait()
        total = zs_send[t]
        for k in range(len(group)):
            total = total + zs_recv[first + k]
        if t + 1 < len(axes):
            zs_send[t + 1] = total
        else:
            rz_ref[...] = 1.0 / total
        first += len(group)

    def drain(ref, sem):
        pltpu.make_async_copy(ref, ref, sem).wait()

    for g, (c0, n) in enumerate(CHUNKS):
        drain(qsrc.at[pl.ds(c0, n), pl.ds(0, nd - 1)], bulk_ss.at[g])

    @pl.when(is_owner)
    def _():
        drain(st_send, st_ss)
        drain(st_send.at[pl.ds(0, nunit - 1)], st_ss)
        drain(st_recv.at[pl.ds(0, nb - 1)], ag_ss)

    @pl.when(jnp.logical_not(is_owner))
    def _():
        drain(st_send, st_ss)
        drain(st_send, st_ss)

    for t, group in enumerate(axes):
        drain(zs_recv.at[pl.ds(0, len(group))], zs_ss.at[t])


def write_out(acc_ref, exp_ref, num_ref, bon_ref, rz_ref, acc_out, exp_out, res_out, bon_out, res, sem):
    nd, per_src = num_ref.shape[:2]
    small = [pltpu.make_async_copy(a, b, sem.at[k]) for k, (a, b) in enumerate(
        ((acc_ref, acc_out), (exp_ref, exp_out), (bon_ref, bon_out)))]
    for c in small:
        c.start()

    def put(c):
        return pltpu.make_async_copy(res.at[:, c], res_out.at[:, c], sem.at[3 + c])

    for c in range(per_src):
        tile = rz_ref[c // 2, (c % 2) * 4:(c % 2) * 4 + 4]
        r8 = jnp.concatenate([tile, tile], axis=0)
        for s in range(nd):
            res[s, c] = num_ref[s, c] * r8[:, s:s + 1]
        put(c).start()
    for c in range(per_src):
        put(c).wait()
    for c in small:
        c.wait()


def solution(mesh):
    na, nb = mesh.shape["tpa"], mesh.shape["tpb"]
    nd = na * nb

    def local_step(hidden, w_head, q_draft, x_draft):
        nseq, npos, dm = hidden.shape
        ndraft = npos - 1
        vloc = w_head.shape[1]
        per_src = q_draft.shape[0]
        nt = vloc // LANES
        h5 = jnp.transpose(hidden, (1, 0, 2))
        q4 = q_draft.reshape(per_src, ndraft, nd, nt, LANES).transpose(0, 2, 3, 1, 4).reshape(per_src, nd, nt * ndraft,
                                                                                             LANES)
        xt = x_draft.T
        nunit = (nseq // LANES) * npos
        hbm = pl.BlockSpec(memory_space=pltpu.HBM)
        vmem = pl.BlockSpec(memory_space=pltpu.VMEM)
        dma, vm = pltpu.SemaphoreType.DMA, pltpu.VMEM
        outs = pl.pallas_call(
            functools.partial(kernel, (na, nb)),
            out_shape=[
                jax.ShapeDtypeStruct((ndraft, nseq), F32),
                jax.ShapeDtypeStruct((1, nseq), F32),
                jax.ShapeDtypeStruct((nseq * nt * ndraft, LANES), F32),
                jax.ShapeDtypeStruct((nseq, vloc), F32),
                jax.ShapeDtypeStruct((per_src // 2, 8, LANES), F32),
            ],
            in_specs=[hbm] * 4,
            out_specs=[vmem] * 5,
            scratch_shapes=[
                vm((NBUF, ROWS, dm), jnp.bfloat16),
                vm((dm, vloc), jnp.bfloat16),
                vm((ndraft, nseq), jnp.int32),
                vm((per_src, nd, 8, LANES), F32),
                vm((nd, per_src, 8, LANES), F32),
                vm((ROWS, vloc), F32),
                vm((nunit, 4, LANES), F32),
                vm((nd, 4, LANES), F32),
                vm((4, LANES), F32),
                vm((nunit, 4, LANES), F32),
                vm((3, per_src // 2, 8, LANES), F32),
                vm((13, per_src // 2, 8, LANES), F32),
                dma((NBUF,)), dma, dma, dma, dma((len(CHUNKS),)), dma((len(CHUNKS),)), dma, dma, dma, dma, dma((3,)),
                dma((3,)),
            ],
            compiler_params=pltpu.CompilerParams(collective_id=0, has_side_effects=True,
                                                 vmem_limit_bytes=46 * 1024 * 1024),
            name="verify",
        )(*[pltpu.with_memory_space_constraint(a, pltpu.HBM) for a in (h5, w_head, q4, xt)])
        acc, exp, num, bonus, rz = outs
        num = num.reshape(nd, per_src, nt * ndraft, LANES)
        outs = (acc, exp, num, bonus)
        acc, exp, res, bonus = pl.pallas_call(
            write_out,
            out_shape=[jax.ShapeDtypeStruct(o.shape, o.dtype) for o in outs],
            in_specs=[vmem] * 5,
            out_specs=[hbm] * 4,
            scratch_shapes=[vm(num.shape, F32), dma((3 + per_src,))],
            compiler_params=pltpu.CompilerParams(vmem_limit_bytes=8 * 1024 * 1024),
            name="write_out",
        )(*outs, rz)
        residual = res.reshape(nseq, nt, ndraft, LANES).transpose(0, 2, 1, 3).reshape(nseq, ndraft, vloc)
        return acc.T, exp.reshape(nseq), residual, bonus

    return jax.shard_map(
        local_step, mesh=mesh,
        in_specs=(P("dp", None, None), P(None, VOCAB_AXES), P(("dp",) + VOCAB_AXES, None, None), P("dp", None)),
        out_specs=(P("dp", None), P("dp"), P("dp", None, VOCAB_AXES), P("dp", VOCAB_AXES)),
        check_vma=False)
```

```python
import functools

import jax
import jax.numpy as jnp
from jax import lax
from jax.experimental import pallas as pl
from jax.experimental.pallas import tpu as pltpu
from jax.sharding import PartitionSpec as P

INV_TEMP = 1.25
VOCAB_AXES = ("tpa", "tpb")
MESH = pl.DeviceIdType.MESH
F32 = jnp.float32
LANES = 128
CHUNKS = ((0, 2), (2, 1), (3, 1), (4, 2), (6, 1), (7, 1))
ROWS = 256
NBUF = 3
EARLY = 3


def kernel(dims, h_ref, w_ref, q_ref, xin_ref, acc_ref, exp_ref, zr, z4, rz_ref,
           hbuf, wbuf, x_ref, qsrc, qdst, zb, st_send, st_part, st_recv, ag_send, ag_recv, zs_send, zs_recv, h_sem, w_sem, q_sem,
           x_sem, bulk_ss, bulk_rs, st_ss, st_rs, ag_ss, ag_rs, pair_ss, pair_rs, zs_ss, zs_rs):
    na, nb = dims
    nd = na * nb
    me_a, me_b = lax.axis_index("tpa"), lax.axis_index("tpb")
    me = me_a * nb + me_b
    npos = h_ref.shape[0]
    ndraft = npos - 1
    nseq = h_ref.shape[1]
    nblk = nseq // LANES
    nunit = nblk * npos
    per_src = nseq // nd
    vloc = w_ref.shape[1]

    def dev(f):
        return {"tpa": f // nb, "tpb": f % nb}

    px, py, pz = me_b % 4, (me_b // 4) % 4, me_b // 16
    xs = [(px + k) % 4 for k in range(4)]
    ys = [((py + k) % 4) * 4 for k in range(4)]
    cores = [me_a, (me_a + 1) % na]

    def each_peer(fn, far=False, own_core=False):
        first = 2 if far else 0

        def plane(kz, carry):
            zz = pz + kz + first
            zz = jnp.where(zz >= 4, zz - 4, zz)
            base = jnp.where(zz >= 4, zz - 4, zz) * 16
            for ky in (2, 1, 3, 0) if far else range(4):
                for kx in (2, 1, 3, 0) if far else (1, 3, 2, 0):
                    for ka in range(1 if own_core else na):
                        b = base + ys[ky] + xs[kx]
                        f = cores[ka] * nb + b
                        ident = {"tpa": cores[ka], "tpb": b}
                        if ka == kx == ky == 0:
                            @pl.when(kz != (4 - first) % 4)
                            def _():
                                fn(f, ident)
                        else:
                            fn(f, ident)
            return carry
        lax.fori_loop(0, 4, plane, 0)

    lane = lax.broadcasted_iota(jnp.int32, (8, LANES), 1)
    sub = lax.broadcasted_iota(jnp.int32, (8, LANES), 0)
    sub4 = lax.broadcasted_iota(jnp.int32, (4, LANES), 0)
    lane_f = lane.astype(F32)
    eye = (lax.broadcasted_iota(jnp.int32, (LANES, LANES), 0) == lax.broadcasted_iota(jnp.int32, (LANES, LANES), 1))

    def to_col(row):
        return jnp.sum(jnp.where(eye, jnp.broadcast_to(row, (LANES, LANES)), 0.0), axis=1, keepdims=True)

    def to_row(col):
        return jnp.sum(jnp.where(eye, jnp.broadcast_to(col, (LANES, LANES)), 0.0), axis=0, keepdims=True)

    def twice(t):
        return jnp.concatenate([t, t], axis=0)

    q_copy = pltpu.make_async_copy(q_ref, qsrc, q_sem)
    q_copy.start()
    w_copy = pltpu.make_async_copy(w_ref, wbuf, w_sem)
    w_copy.start()
    per_pos = nseq // ROWS

    def h_copy(t):
        return pltpu.make_async_copy(h_ref.at[t // per_pos, pl.ds((t % per_pos) * ROWS, ROWS)], hbuf.at[t % NBUF],
                                     h_sem.at[t % NBUF])

    x_copy = pltpu.make_async_copy(xin_ref, x_ref, x_sem)
    x_copy.start()
    for t in range(NBUF - 1):
        h_copy(t).start()

    barrier = pltpu.get_barrier_semaphore()
    each_peer(lambda f, ident: pl.semaphore_signal(barrier, inc=1, device_id=ident, device_id_type=MESH), far=True)
    q_copy.wait()

    def local_bulk(g):
        c0, n = CHUNKS[g]
        return pltpu.make_async_copy(qsrc.at[pl.ds(c0, n), me], qdst.at[me, pl.ds(c0, n)], bulk_rs.at[g])

    for g in range(len(CHUNKS)):
        local_bulk(g).start()
    x_copy.wait()
    xb = x_ref[:, pl.ds(pl.multiple_of((me // 16) * LANES, LANES), LANES)].astype(F32)
    targets = []
    for c in range(per_src):
        j = (me % 16) * per_src + c
        col = jnp.sum(jnp.where(lane[:4] == j, xb, 0.0), axis=1, keepdims=True)
        targets.append(twice(jnp.broadcast_to(col, (4, LANES))) - jnp.where(sub >= 4, F32(LANES), F32(0)) - lane_f)

    def pick_q(d, accs):
        base = (d * vloc).astype(F32)
        return tuple(a + jnp.where(t == base, qsrc[c, d], 0.0) for c, (a, t) in enumerate(zip(accs, targets)))

    accs = lax.fori_loop(0, nd, pick_q, tuple(jnp.zeros((8, LANES), F32) for _ in range(per_src)),
                         unroll=8)
    qp = jnp.zeros((4, LANES), F32)
    for c in range(per_src):
        col = jnp.sum(accs[c], axis=1, keepdims=True)
        qp = jnp.where(lane[:4] == (me % 16) * per_src + c, col[:4] + col[4:], qp)


    def send_bulk(g):
        c0, n = CHUNKS[g]

        def one(c, carry):
            each_peer(lambda f, ident: pltpu.make_async_remote_copy(
                src_ref=qsrc.at[c, f], dst_ref=qdst.at[me, c], send_sem=bulk_ss.at[g], recv_sem=bulk_rs.at[g],
                device_id=ident, device_id_type=MESH).start())
            return carry

        lax.fori_loop(c0, c0 + n, one, 0)

    def wait_bulk(g):
        c0, n = CHUNKS[g]
        ref = qdst.at[:, pl.ds(c0, n)]
        pltpu.make_async_copy(ref, ref, bulk_rs.at[g]).wait()

    w_copy.wait()
    my_base = (me * vloc).astype(F32)
    lane2 = lax.broadcasted_iota(jnp.int32, (LANES, vloc), 1).astype(F32)

    def matmul(t, carry):
        @pl.when(t + NBUF - 1 < npos * per_pos)
        def _():
            h_copy(t + NBUF - 1).start()

        h_copy(t).wait()
        i, r = t // per_pos, t % per_pos
        zb[...] = jnp.dot(hbuf[t % NBUF], wbuf[...], preferred_element_type=F32) * INV_TEMP
        for half in range(ROWS // LANES):
            blk = r * (ROWS // LANES) + half
            zz = zb[half * LANES:(half + 1) * LANES, :]
            m = jnp.max(zz, axis=1, keepdims=True)
            s = jnp.sum(jnp.exp(zz - m), axis=1, keepdims=True)
            ii = jnp.minimum(i, ndraft - 1)
            xblk = x_ref[:, pl.ds(pl.multiple_of(blk * LANES, LANES), LANES)].astype(F32)
            xrow = jnp.sum(jnp.where(sub4 == ii, xblk, 0.0), axis=0, keepdims=True) - my_base
            pick = jnp.sum(jnp.where(lane2 == to_col(xrow), zz, 0.0), axis=1, keepdims=True)
            qrow = jnp.sum(jnp.where((sub4 == ii) & (blk == me // 16), qp, 0.0), axis=0, keepdims=True)
            tile = jnp.where(sub4 == 0, to_row(m), jnp.where(sub4 == 1, to_row(s), jnp.where(
                sub4 == 2, to_row(pick), qrow)))
            st_send[blk * npos + i] = tile

            @pl.when(i < ndraft)
            def _():
                for lt in range(vloc // LANES):
                    zr[pl.ds(blk * LANES * 8 + lt * 4 + i, LANES, stride=8), :] = zz[:, lt * LANES:(lt + 1) * LANES]

            @pl.when(i == ndraft)
            def _():
                z4[pl.ds(pl.multiple_of(blk * LANES, LANES), LANES), :] = zz
        return carry

    lax.fori_loop(0, EARLY, matmul, 0)
    pl.semaphore_wait(barrier, nd - 1)
    send_bulk(0)

    @pl.when(me_a == 0)
    def _():
        send_bulk(1)

    lax.fori_loop(EARLY, npos * per_pos, matmul, 0)

    my_unit = (me_b * 43) % nb
    is_owner = (my_unit < nunit) & (me_a == 1)
    partner = {"tpa": cores[1], "tpb": me_b}
    pair_stats = pltpu.make_async_remote_copy(src_ref=st_send, dst_ref=st_part, send_sem=pair_ss, recv_sem=pair_rs,
                                              device_id=partner, device_id_type=MESH)
    pair_answers = pltpu.make_async_remote_copy(src_ref=ag_recv, dst_ref=ag_recv, send_sem=pair_ss, recv_sem=ag_rs,
                                                device_id=partner, device_id_type=MESH)

    @pl.when(me_a == 0)
    def _():
        pair_stats.start()
        for g in range(2, len(CHUNKS)):
            send_bulk(g)

    def merge(u, carry):
        mine, other = st_send[u], st_part[u]
        top = jnp.maximum(mine[0:1], other[0:1])
        total = mine[1:2] * jnp.exp(mine[0:1] - top) + other[1:2] * jnp.exp(other[0:1] - top)
        st_send[u] = jnp.where(sub4 == 0, top, jnp.where(sub4 == 1, total, mine + other))
        return carry

    def send_stats(u, carry):
        chip = (u * 3) % nb

        @pl.when(chip != me_b)
        def _():
            pltpu.make_async_remote_copy(src_ref=st_send.at[u], dst_ref=st_recv.at[me_b], send_sem=st_ss,
                                         recv_sem=st_rs, device_id={"tpa": me_a, "tpb": chip},
                                         device_id_type=MESH).start()
        return carry

    @pl.when(me_a == 1)
    def _():
        pair_stats.wait_recv()
        lax.fori_loop(0, nunit, merge, 0, unroll=4)
        lax.fori_loop(0, nunit, send_stats, 0)
        send_bulk(1)

        @pl.when(is_owner)
        def _():
            pltpu.make_async_copy(st_send.at[my_unit], st_recv.at[me_b], st_rs).start()
            pltpu.make_async_copy(st_recv, st_recv, st_rs).wait()
            mx = lax.fori_loop(0, nb, lambda s, m: jnp.maximum(m, st_recv[s]), st_recv[0], unroll=8)[0:1]

            def add(s, carry):
                t = st_recv[s]
                es, zp, qq = carry
                return es + jnp.exp(t[0:1] - mx) * t[1:2], zp + t[2:3], qq + t[3:4]

            zero = jnp.zeros((1, LANES), F32)
            es, zp, qq = lax.fori_loop(0, nb, add, (zero, zero, zero), unroll=8)
            accept = jnp.minimum(1.0, jnp.exp(zp - mx) / es / qq)
            ag_send[...] = jnp.where(sub4 == 0, mx, jnp.where(sub4 == 1, 1.0 / es, accept))
            pltpu.make_async_copy(ag_send, ag_recv.at[my_unit], ag_rs).start()
            each_peer(lambda f, ident: pltpu.make_async_remote_copy(
                src_ref=ag_send, dst_ref=ag_recv.at[my_unit], send_sem=ag_ss, recv_sem=ag_rs, device_id=ident,
                device_id_type=MESH).start(), far=True, own_core=True)

    pltpu.make_async_copy(ag_recv, ag_recv, ag_rs).wait()

    @pl.when(me_a == 1)
    def _():
        pair_answers.start()
        for g in range(2, len(CHUNKS)):
            send_bulk(g)

    def stat_rows(blk, k):
        return jnp.concatenate([ag_recv[blk * npos + i, k:k + 1, :] for i in range(ndraft)], axis=0)

    def probs(c0, n):
        def body(blk, carry):
            m8, r8 = twice(stat_rows(blk, 0)), twice(stat_rows(blk, 1))
            for j in range(LANES):
                if c0 <= j % per_src < c0 + n:
                    at = pl.ds(pl.multiple_of((blk * LANES + j) * 8, 8), 8)
                    zr[at, :] = jnp.exp(zr[at, :] - m8[:, j:j + 1]) * r8[:, j:j + 1]
            return carry
        lax.fori_loop(0, nblk, body, 0)

    def verdicts(blk, carry):
        a4 = stat_rows(blk, 2)
        cols = pl.ds(pl.multiple_of(blk * LANES, LANES), LANES)
        acc_ref[:, cols] = a4
        run, tot = a4[0:1], a4[0:1]
        for i in range(1, ndraft):
            run = run * a4[i:i + 1]
            tot = tot + run
        exp_ref[:, cols] = tot
        u4 = blk * npos + ndraft
        z4[cols, :] = jnp.exp(z4[cols, :] - to_col(ag_recv[u4, 0:1, :])) * to_col(ag_recv[u4, 1:2, :])
        return carry

    def excess(g):
        c0, n = CHUNKS[g]

        def body(s, accs):
            new = []
            for c in range(n):
                at = pl.ds(pl.multiple_of((s * per_src + c0 + c) * 8, 8), 8)
                e = jnp.maximum(zr[at, :] - qdst[s, c0 + c], 0.0)
                zr[at, :] = e
                new.append(jnp.where(lane == s, jnp.sum(e, axis=1, keepdims=True), accs[c]))
            return tuple(new)

        accs = lax.fori_loop(0, nd, body, tuple(jnp.zeros((8, LANES), F32) for _ in range(n)), unroll=4)
        for c in range(n):
            part = accs[c][:4] + accs[c][4:]
            zs_send[0, (c0 + c) // 2, ((c0 + c) % 2) * 4:((c0 + c) % 2) * 4 + 4] = part

    half = CHUNKS[3][0]
    probs(0, half)
    for g in range(3):
        wait_bulk(g)
        excess(g)
    probs(half, per_src - half)
    for g in range(3, len(CHUNKS)):
        wait_bulk(g)
        excess(g)

    axes = [[{"tpa": cores[a], "tpb": me_b - px + xs[k]} for k in (2, 1, 3, 0) for a in range(na) if (k, a) != (0, 0)],
            [{"tpa": me_a, "tpb": me_b - py * 4 + ys[k]} for k in (2, 1, 3)],
            [{"tpa": me_a, "tpb": me_b - pz * 16 + ((pz + k) % 4) * 16} for k in (2, 1, 3)]]
    first = 0
    for t, group in enumerate(axes):
        for k, ident in enumerate(group):
            pltpu.make_async_remote_copy(src_ref=zs_send.at[t], dst_ref=zs_recv.at[first + k], send_sem=zs_ss.at[t],
                                         recv_sem=zs_rs.at[t], device_id=ident, device_id_type=MESH).start()
        if t == 0:
            lax.fori_loop(0, nblk, verdicts, 0)
        ref = zs_recv.at[pl.ds(first, len(group))]
        pltpu.make_async_copy(ref, ref, zs_rs.at[t]).wait()
        total = zs_send[t]
        for k in range(len(group)):
            total = total + zs_recv[first + k]
        if t + 1 < len(axes):
            zs_send[t + 1] = total
        else:
            rz_ref[...] = 1.0 / total
        first += len(group)

    def drain(ref, sem):
        pltpu.make_async_copy(ref, ref, sem).wait()

    for g, (c0, n) in enumerate(CHUNKS):
        drain(qsrc.at[pl.ds(c0, n), pl.ds(0, nd - 1)], bulk_ss.at[g])

    drain(st_send, pair_ss)

    @pl.when(is_owner)
    def _():
        drain(st_send.at[pl.ds(0, nunit - 1)], st_ss)
        drain(st_recv.at[pl.ds(0, nb - 1)], ag_ss)

    @pl.when(jnp.logical_not(is_owner) & (me_a == 1))
    def _():
        drain(st_send, st_ss)

    for t, group in enumerate(axes):
        drain(zs_recv.at[pl.ds(0, len(group))], zs_ss.at[t])


def write_out(acc_ref, exp_ref, num_ref, bon_ref, rz_ref, acc_out, exp_out, res_out, bon_out, res, sem):
    nd, per_src = num_ref.shape[:2]
    small = [pltpu.make_async_copy(a, b, sem.at[k]) for k, (a, b) in enumerate(
        ((acc_ref, acc_out), (exp_ref, exp_out), (bon_ref, bon_out)))]
    for c in small:
        c.start()

    def put(c):
        return pltpu.make_async_copy(res.at[:, c], res_out.at[:, c], sem.at[3 + c])

    for c in range(per_src):
        tile = rz_ref[c // 2, (c % 2) * 4:(c % 2) * 4 + 4]
        r8 = jnp.concatenate([tile, tile], axis=0)
        for s in range(nd):
            res[s, c] = num_ref[s, c] * r8[:, s:s + 1]
        put(c).start()
    for c in range(per_src):
        put(c).wait()
    for c in small:
        c.wait()


def solution(mesh):
    na, nb = mesh.shape["tpa"], mesh.shape["tpb"]
    nd = na * nb

    def local_step(hidden, w_head, q_draft, x_draft):
        nseq, npos, dm = hidden.shape
        ndraft = npos - 1
        vloc = w_head.shape[1]
        per_src = q_draft.shape[0]
        nt = vloc // LANES
        h5 = jnp.transpose(hidden, (1, 0, 2))
        q4 = q_draft.reshape(per_src, ndraft, nd, nt, LANES).transpose(0, 2, 3, 1, 4).reshape(per_src, nd, nt * ndraft,
                                                                                             LANES)
        xt = x_draft.T
        nunit = (nseq // LANES) * npos
        hbm = pl.BlockSpec(memory_space=pltpu.HBM)
        vmem = pl.BlockSpec(memory_space=pltpu.VMEM)
        dma, vm = pltpu.SemaphoreType.DMA, pltpu.VMEM
        outs = pl.pallas_call(
            functools.partial(kernel, (na, nb)),
            out_shape=[
                jax.ShapeDtypeStruct((ndraft, nseq), F32),
                jax.ShapeDtypeStruct((1, nseq), F32),
                jax.ShapeDtypeStruct((nseq * nt * ndraft, LANES), F32),
                jax.ShapeDtypeStruct((nseq, vloc), F32),
                jax.ShapeDtypeStruct((per_src // 2, 8, LANES), F32),
            ],
            in_specs=[hbm] * 4,
            out_specs=[vmem] * 5,
            scratch_shapes=[
                vm((NBUF, ROWS, dm), jnp.bfloat16),
                vm((dm, vloc), jnp.bfloat16),
                vm((ndraft, nseq), jnp.int32),
                vm((per_src, nd, 8, LANES), F32),
                vm((nd, per_src, 8, LANES), F32),
                vm((ROWS, vloc), F32),
                vm((nunit, 4, LANES), F32),
                vm((nunit, 4, LANES), F32),
                vm((nb, 4, LANES), F32),
                vm((4, LANES), F32),
                vm((nunit, 4, LANES), F32),
                vm((3, per_src // 2, 8, LANES), F32),
                vm((13, per_src // 2, 8, LANES), F32),
                dma((NBUF,)), dma, dma, dma, dma((len(CHUNKS),)), dma((len(CHUNKS),)), dma, dma, dma, dma, dma, dma,
                dma((3,)), dma((3,)),
            ],
            compiler_params=pltpu.CompilerParams(collective_id=0, has_side_effects=True,
                                                 vmem_limit_bytes=46 * 1024 * 1024),
            name="verify",
        )(*[pltpu.with_memory_space_constraint(a, pltpu.HBM) for a in (h5, w_head, q4, xt)])
        acc, exp, num, bonus, rz = outs
        num = num.reshape(nd, per_src, nt * ndraft, LANES)
        outs = (acc, exp, num, bonus)
        acc, exp, res, bonus = pl.pallas_call(
            write_out,
            out_shape=[jax.ShapeDtypeStruct(o.shape, o.dtype) for o in outs],
            in_specs=[vmem] * 5,
            out_specs=[hbm] * 4,
            scratch_shapes=[vm(num.shape, F32), dma((3 + per_src,))],
            compiler_params=pltpu.CompilerParams(vmem_limit_bytes=8 * 1024 * 1024),
            name="write_out",
        )(*outs, rz)
        residual = res.reshape(nseq, nt, ndraft, LANES).transpose(0, 2, 1, 3).reshape(nseq, ndraft, vloc)
        return acc.T, exp.reshape(nseq), residual, bonus

    return jax.shard_map(
        local_step, mesh=mesh,
        in_specs=(P("dp", None, None), P(None, VOCAB_AXES), P(("dp",) + VOCAB_AXES, None, None), P("dp", None)),
        out_specs=(P("dp", None), P("dp"), P("dp", None, VOCAB_AXES), P("dp", VOCAB_AXES)),
        check_vma=False)
```

```python
import functools

import jax
import jax.numpy as jnp
from jax import lax
from jax.experimental import pallas as pl
from jax.experimental.pallas import tpu as pltpu
from jax.sharding import PartitionSpec as P

INV_TEMP = 1.25
VOCAB_AXES = ("tpa", "tpb")
MESH = pl.DeviceIdType.MESH
F32 = jnp.float32
LANES = 128
CHUNKS = ((0, 4), (4, 1), (5, 1), (6, 1), (7, 1))
ROWS = 256
NBUF = 6
EARLY = 3


def kernel(dims, h_ref, w_ref, q_ref, xin_ref, acc_ref, exp_ref, zr, z4, rz_ref,
           hbuf, wbuf, x_ref, qsrc, qdst, zb, st_send, st_recv, ag_send, ag_recv, zs_send, zs_recv, h_sem, w_sem, q_sem,
           x_sem, bulk_ss, bulk_rs, st_ss, st_rs, ag_ss, ag_rs, zs_ss, zs_rs):
    na, nb = dims
    nd = na * nb
    me_a, me_b = lax.axis_index("tpa"), lax.axis_index("tpb")
    me = me_a * nb + me_b
    npos = h_ref.shape[0]
    ndraft = npos - 1
    nseq = h_ref.shape[1]
    nblk = nseq // LANES
    nunit = nblk * npos
    per_src = nseq // nd
    vloc = w_ref.shape[1]

    def dev(f):
        return {"tpa": f // nb, "tpb": f % nb}

    px, py, pz = me_b % 4, (me_b // 4) % 4, me_b // 16
    xs = [(px + k) % 4 for k in range(4)]
    ys = [((py + k) % 4) * 4 for k in range(4)]
    cores = [me_a, (me_a + 1) % na]

    def each_peer(fn, far=False, own_core=False):
        first = 2 if far else 0

        def plane(kz, carry):
            zz = pz + kz + first
            zz = jnp.where(zz >= 4, zz - 4, zz)
            base = jnp.where(zz >= 4, zz - 4, zz) * 16
            for ky in (2, 1, 3, 0) if far else range(4):
                for kx in (2, 1, 3, 0) if far else (1, 3, 2, 0):
                    for ka in range(1 if own_core else na):
                        b = base + ys[ky] + xs[kx]
                        f = cores[ka] * nb + b
                        ident = {"tpa": cores[ka], "tpb": b}
                        if ka == kx == ky == 0:
                            @pl.when(kz != (4 - first) % 4)
                            def _():
                                fn(f, ident)
                        else:
                            fn(f, ident)
            return carry
        lax.fori_loop(0, 4, plane, 0)

    lane = lax.broadcasted_iota(jnp.int32, (8, LANES), 1)
    sub = lax.broadcasted_iota(jnp.int32, (8, LANES), 0)
    sub4 = lax.broadcasted_iota(jnp.int32, (4, LANES), 0)
    lane_f = lane.astype(F32)
    eye = (lax.broadcasted_iota(jnp.int32, (LANES, LANES), 0) == lax.broadcasted_iota(jnp.int32, (LANES, LANES), 1))

    def to_col(row):
        return jnp.sum(jnp.where(eye, jnp.broadcast_to(row, (LANES, LANES)), 0.0), axis=1, keepdims=True)

    def to_row(col):
        return jnp.sum(jnp.where(eye, jnp.broadcast_to(col, (LANES, LANES)), 0.0), axis=0, keepdims=True)

    def twice(t):
        return jnp.concatenate([t, t], axis=0)

    q_copy = pltpu.make_async_copy(q_ref, qsrc, q_sem)
    q_copy.start()
    w_copy = pltpu.make_async_copy(w_ref, wbuf, w_sem)
    w_copy.start()
    per_pos = nseq // ROWS

    def h_copy(t):
        return pltpu.make_async_copy(h_ref.at[t // per_pos, pl.ds((t % per_pos) * ROWS, ROWS)], hbuf.at[t % NBUF],
                                     h_sem.at[t % NBUF])

    x_copy = pltpu.make_async_copy(xin_ref, x_ref, x_sem)
    x_copy.start()
    for t in range(NBUF - 1):
        h_copy(t).start()

    barrier = pltpu.get_barrier_semaphore()
    each_peer(lambda f, ident: pl.semaphore_signal(barrier, inc=1, device_id=ident, device_id_type=MESH), far=True)
    q_copy.wait()

    def local_bulk(g):
        c0, n = CHUNKS[g]
        return pltpu.make_async_copy(qsrc.at[pl.ds(c0, n), me], qdst.at[me, pl.ds(c0, n)], bulk_rs.at[g])

    for g in range(len(CHUNKS)):
        local_bulk(g).start()
    x_copy.wait()
    xb = x_ref[:, pl.ds(pl.multiple_of((me // 16) * LANES, LANES), LANES)].astype(F32)
    targets = []
    for c in range(per_src):
        j = (me % 16) * per_src + c
        col = jnp.sum(jnp.where(lane[:4] == j, xb, 0.0), axis=1, keepdims=True)
        targets.append(twice(jnp.broadcast_to(col, (4, LANES))) - jnp.where(sub >= 4, F32(LANES), F32(0)) - lane_f)

    def pick_q(d, accs):
        base = (d * vloc).astype(F32)
        return tuple(a + jnp.where(t == base, qsrc[c, d], 0.0) for c, (a, t) in enumerate(zip(accs, targets)))

    accs = lax.fori_loop(0, nd, pick_q, tuple(jnp.zeros((8, LANES), F32) for _ in range(per_src)),
                         unroll=8)
    qp = jnp.zeros((4, LANES), F32)
    for c in range(per_src):
        col = jnp.sum(accs[c], axis=1, keepdims=True)
        qp = jnp.where(lane[:4] == (me % 16) * per_src + c, col[:4] + col[4:], qp)


    def send_bulk(g):
        c0, n = CHUNKS[g]

        def one(c, carry):
            each_peer(lambda f, ident: pltpu.make_async_remote_copy(
                src_ref=qsrc.at[c, f], dst_ref=qdst.at[me, c], send_sem=bulk_ss.at[g], recv_sem=bulk_rs.at[g],
                device_id=ident, device_id_type=MESH).start())
            return carry

        lax.fori_loop(c0, c0 + n, one, 0)

    def wait_bulk(g):
        c0, n = CHUNKS[g]
        ref = qdst.at[:, pl.ds(c0, n)]
        pltpu.make_async_copy(ref, ref, bulk_rs.at[g]).wait()

    w_copy.wait()
    my_base = (me * vloc).astype(F32)
    lane2 = lax.broadcasted_iota(jnp.int32, (LANES, vloc), 1).astype(F32)

    def matmul(t, carry):
        @pl.when(t + NBUF - 1 < npos * per_pos)
        def _():
            h_copy(t + NBUF - 1).start()

        h_copy(t).wait()
        i, r = t // per_pos, t % per_pos
        zb[...] = jnp.dot(hbuf[t % NBUF], wbuf[...], preferred_element_type=F32) * INV_TEMP
        for half in range(ROWS // LANES):
            blk = r * (ROWS // LANES) + half
            zz = zb[half * LANES:(half + 1) * LANES, :]
            m = jnp.max(zz, axis=1, keepdims=True)
            s = jnp.sum(jnp.exp(zz - m), axis=1, keepdims=True)
            ii = jnp.minimum(i, ndraft - 1)
            xblk = x_ref[:, pl.ds(pl.multiple_of(blk * LANES, LANES), LANES)].astype(F32)
            xrow = jnp.sum(jnp.where(sub4 == ii, xblk, 0.0), axis=0, keepdims=True) - my_base
            pick = jnp.sum(jnp.where(lane2 == to_col(xrow), zz, 0.0), axis=1, keepdims=True)
            qrow = jnp.sum(jnp.where((sub4 == ii) & (blk == me // 16), qp, 0.0), axis=0, keepdims=True)
            tile = jnp.where(sub4 == 0, to_row(m), jnp.where(sub4 == 1, to_row(s), jnp.where(
                sub4 == 2, to_row(pick), qrow)))
            st_send[blk * npos + i] = tile

            @pl.when(i < ndraft)
            def _():
                for lt in range(vloc // LANES):
                    zr[pl.ds(blk * LANES * 8 + lt * 4 + i, LANES, stride=8), :] = zz[:, lt * LANES:(lt + 1) * LANES]

            @pl.when(i == ndraft)
            def _():
                z4[pl.ds(pl.multiple_of(blk * LANES, LANES), LANES), :] = zz
        return carry

    lax.fori_loop(0, EARLY, matmul, 0)
    pl.semaphore_wait(barrier, nd - 1)
    send_bulk(0)
    lax.fori_loop(EARLY, npos * per_pos, matmul, 0)

    my_unit = (me_b * 43) % nb
    is_owner = my_unit < nunit

    def send_stats(u, carry):
        chip = (u * 3) % nb
        for a in range(na):
            @pl.when((chip != me_b) | (me_a != a))
            def _():
                pltpu.make_async_remote_copy(src_ref=st_send.at[u], dst_ref=st_recv.at[me], send_sem=st_ss,
                                             recv_sem=st_rs, device_id={"tpa": a, "tpb": chip},
                                             device_id_type=MESH).start()
        return carry

    lax.fori_loop(0, nunit, send_stats, 0)
    send_bulk(1)

    @pl.when(is_owner)
    def _():
        pltpu.make_async_copy(st_send.at[my_unit], st_recv.at[me], st_rs).start()
        pltpu.make_async_copy(st_recv, st_recv, st_rs).wait()
        mx = lax.fori_loop(0, nd, lambda s, m: jnp.maximum(m, st_recv[s]), st_recv[0], unroll=8)[0:1]

        def add(s, carry):
            t = st_recv[s]
            es, zp, qq = carry
            return es + jnp.exp(t[0:1] - mx) * t[1:2], zp + t[2:3], qq + t[3:4]

        zero = jnp.zeros((1, LANES), F32)
        es, zp, qq = lax.fori_loop(0, nd, add, (zero, zero, zero), unroll=8)
        accept = jnp.minimum(1.0, jnp.exp(zp - mx) / es / qq)
        ag_send[...] = jnp.where(sub4 == 0, mx, jnp.where(sub4 == 1, 1.0 / es, accept))
        pltpu.make_async_copy(ag_send, ag_recv.at[my_unit], ag_rs).start()
        each_peer(lambda f, ident: pltpu.make_async_remote_copy(
            src_ref=ag_send, dst_ref=ag_recv.at[my_unit], send_sem=ag_ss, recv_sem=ag_rs, device_id=ident,
            device_id_type=MESH).start(), far=True, own_core=True)

    send_bulk(2)

    pltpu.make_async_copy(ag_recv, ag_recv, ag_rs).wait()
    for g in range(3, len(CHUNKS)):
        send_bulk(g)

    def stat_rows(blk, k):
        return jnp.concatenate([ag_recv[blk * npos + i, k:k + 1, :] for i in range(ndraft)], axis=0)

    def probs(c0, n):
        def body(blk, carry):
            m8, r8 = twice(stat_rows(blk, 0)), twice(stat_rows(blk, 1))
            for j in range(LANES):
                if c0 <= j % per_src < c0 + n:
                    at = pl.ds(pl.multiple_of((blk * LANES + j) * 8, 8), 8)
                    zr[at, :] = jnp.exp(zr[at, :] - m8[:, j:j + 1]) * r8[:, j:j + 1]
            return carry
        lax.fori_loop(0, nblk, body, 0)

    def verdicts(blk, carry):
        a4 = stat_rows(blk, 2)
        cols = pl.ds(pl.multiple_of(blk * LANES, LANES), LANES)
        acc_ref[:, cols] = a4
        run, tot = a4[0:1], a4[0:1]
        for i in range(1, ndraft):
            run = run * a4[i:i + 1]
            tot = tot + run
        exp_ref[:, cols] = tot
        u4 = blk * npos + ndraft
        z4[cols, :] = jnp.exp(z4[cols, :] - to_col(ag_recv[u4, 0:1, :])) * to_col(ag_recv[u4, 1:2, :])
        return carry

    def excess(g):
        c0, n = CHUNKS[g]

        def body(s, accs):
            new = []
            for c in range(n):
                at = pl.ds(pl.multiple_of((s * per_src + c0 + c) * 8, 8), 8)
                e = jnp.maximum(zr[at, :] - qdst[s, c0 + c], 0.0)
                zr[at, :] = e
                new.append(jnp.where(lane == s, jnp.sum(e, axis=1, keepdims=True), accs[c]))
            return tuple(new)

        accs = lax.fori_loop(0, nd, body, tuple(jnp.zeros((8, LANES), F32) for _ in range(n)), unroll=4)
        for c in range(n):
            part = accs[c][:4] + accs[c][4:]
            zs_send[0, (c0 + c) // 2, ((c0 + c) % 2) * 4:((c0 + c) % 2) * 4 + 4] = part

    half = CHUNKS[2][0]
    probs(0, half)
    for g in range(2):
        wait_bulk(g)
        excess(g)
    probs(half, per_src - half)
    for g in range(2, len(CHUNKS)):
        wait_bulk(g)
        excess(g)

    axes = [[{"tpa": cores[a], "tpb": me_b - px + xs[k]} for k in (2, 1, 3, 0) for a in range(na) if (k, a) != (0, 0)],
            [{"tpa": me_a, "tpb": me_b - py * 4 + ys[k]} for k in (2, 1, 3)],
            [{"tpa": me_a, "tpb": me_b - pz * 16 + ((pz + k) % 4) * 16} for k in (2, 1, 3)]]
    first = 0
    for t, group in enumerate(axes):
        for k, ident in enumerate(group):
            pltpu.make_async_remote_copy(src_ref=zs_send.at[t], dst_ref=zs_recv.at[first + k], send_sem=zs_ss.at[t],
                                         recv_sem=zs_rs.at[t], device_id=ident, device_id_type=MESH).start()
        if t == 0:
            lax.fori_loop(0, nblk, verdicts, 0)
        ref = zs_recv.at[pl.ds(first, len(group))]
        pltpu.make_async_copy(ref, ref, zs_rs.at[t]).wait()
        total = zs_send[t]
        for k in range(len(group)):
            total = total + zs_recv[first + k]
        if t + 1 < len(axes):
            zs_send[t + 1] = total
        else:
            rz_ref[...] = 1.0 / total
        first += len(group)

    def drain(ref, sem):
        pltpu.make_async_copy(ref, ref, sem).wait()

    for g, (c0, n) in enumerate(CHUNKS):
        drain(qsrc.at[pl.ds(c0, n), pl.ds(0, nd - 1)], bulk_ss.at[g])

    @pl.when(is_owner)
    def _():
        drain(st_send, st_ss)
        drain(st_send.at[pl.ds(0, nunit - 1)], st_ss)
        drain(st_recv.at[pl.ds(0, nb - 1)], ag_ss)

    @pl.when(jnp.logical_not(is_owner))
    def _():
        drain(st_send, st_ss)
        drain(st_send, st_ss)

    for t, group in enumerate(axes):
        drain(zs_recv.at[pl.ds(0, len(group))], zs_ss.at[t])


def write_out(acc_ref, exp_ref, num_ref, bon_ref, rz_ref, acc_out, exp_out, res_out, bon_out, res, sem):
    nd, per_src = num_ref.shape[:2]
    small = [pltpu.make_async_copy(a, b, sem.at[k]) for k, (a, b) in enumerate(
        ((acc_ref, acc_out), (exp_ref, exp_out), (bon_ref, bon_out)))]
    for c in small:
        c.start()

    def put(c):
        return pltpu.make_async_copy(res.at[:, c], res_out.at[:, c], sem.at[3 + c])

    for c in range(per_src):
        tile = rz_ref[c // 2, (c % 2) * 4:(c % 2) * 4 + 4]
        r8 = jnp.concatenate([tile, tile], axis=0)
        for s in range(nd):
            res[s, c] = num_ref[s, c] * r8[:, s:s + 1]
        put(c).start()
    for c in range(per_src):
        put(c).wait()
    for c in small:
        c.wait()


def solution(mesh):
    na, nb = mesh.shape["tpa"], mesh.shape["tpb"]
    nd = na * nb

    def local_step(hidden, w_head, q_draft, x_draft):
        nseq, npos, dm = hidden.shape
        ndraft = npos - 1
        vloc = w_head.shape[1]
        per_src = q_draft.shape[0]
        nt = vloc // LANES
        h5 = jnp.transpose(hidden, (1, 0, 2))
        q4 = q_draft.reshape(per_src, ndraft, nd, nt, LANES).transpose(0, 2, 3, 1, 4).reshape(per_src, nd, nt * ndraft,
                                                                                             LANES)
        xt = x_draft.T
        nunit = (nseq // LANES) * npos
        hbm = pl.BlockSpec(memory_space=pltpu.HBM)
        vmem = pl.BlockSpec(memory_space=pltpu.VMEM)
        dma, vm = pltpu.SemaphoreType.DMA, pltpu.VMEM
        outs = pl.pallas_call(
            functools.partial(kernel, (na, nb)),
            out_shape=[
                jax.ShapeDtypeStruct((ndraft, nseq), F32),
                jax.ShapeDtypeStruct((1, nseq), F32),
                jax.ShapeDtypeStruct((nseq * nt * ndraft, LANES), F32),
                jax.ShapeDtypeStruct((nseq, vloc), F32),
                jax.ShapeDtypeStruct((per_src // 2, 8, LANES), F32),
            ],
            in_specs=[hbm] * 4,
            out_specs=[vmem] * 5,
            scratch_shapes=[
                vm((NBUF, ROWS, dm), jnp.bfloat16),
                vm((dm, vloc), jnp.bfloat16),
                vm((ndraft, nseq), jnp.int32),
                vm((per_src, nd, 8, LANES), F32),
                vm((nd, per_src, 8, LANES), F32),
                vm((ROWS, vloc), F32),
                vm((nunit, 4, LANES), F32),
                vm((nd, 4, LANES), F32),
                vm((4, LANES), F32),
                vm((nunit, 4, LANES), F32),
                vm((3, per_src // 2, 8, LANES), F32),
                vm((13, per_src // 2, 8, LANES), F32),
                dma((NBUF,)), dma, dma, dma, dma((len(CHUNKS),)), dma((len(CHUNKS),)), dma, dma, dma, dma, dma((3,)),
                dma((3,)),
            ],
            compiler_params=pltpu.CompilerParams(collective_id=0, has_side_effects=True,
                                                 vmem_limit_bytes=46 * 1024 * 1024),
            name="verify",
        )(*[pltpu.with_memory_space_constraint(a, pltpu.HBM) for a in (h5, w_head, q4, xt)])
        acc, exp, num, bonus, rz = outs
        num = num.reshape(nd, per_src, nt * ndraft, LANES)
        outs = (acc, exp, num, bonus)
        acc, exp, res, bonus = pl.pallas_call(
            write_out,
            out_shape=[jax.ShapeDtypeStruct(o.shape, o.dtype) for o in outs],
            in_specs=[vmem] * 5,
            out_specs=[hbm] * 4,
            scratch_shapes=[vm(num.shape, F32), dma((3 + per_src,))],
            compiler_params=pltpu.CompilerParams(vmem_limit_bytes=8 * 1024 * 1024),
            name="write_out",
        )(*outs, rz)
        residual = res.reshape(nseq, nt, ndraft, LANES).transpose(0, 2, 1, 3).reshape(nseq, ndraft, vloc)
        return acc.T, exp.reshape(nseq), residual, bonus

    return jax.shard_map(
        local_step, mesh=mesh,
        in_specs=(P("dp", None, None), P(None, VOCAB_AXES), P(("dp",) + VOCAB_AXES, None, None), P("dp", None)),
        out_specs=(P("dp", None), P("dp"), P("dp", None, VOCAB_AXES), P("dp", VOCAB_AXES)),
        check_vma=False)
```

```python
import functools

import jax
import jax.numpy as jnp
from jax import lax
from jax.experimental import pallas as pl
from jax.experimental.pallas import tpu as pltpu
from jax.sharding import PartitionSpec as P

INV_TEMP = 1.25
VOCAB_AXES = ("tpa", "tpb")
MESH = pl.DeviceIdType.MESH
F32 = jnp.float32
LANES = 128
CHUNKS = ((0, 2), (2, 1), (3, 2), (5, 2), (7, 1))
ROWS = 256
NBUF = 3
EARLY = 3


def kernel(dims, h_ref, w_ref, q_ref, xin_ref, acc_ref, exp_ref, zr, z4, rz_ref,
           hbuf, wbuf, x_ref, qsrc, qdst, zb, st_send, st_recv, ag_send, ag_recv, zs_send, zs_recv, h_sem, w_sem, q_sem,
           x_sem, bulk_ss, bulk_rs, st_ss, st_rs, ag_ss, ag_rs, zs_ss, zs_rs):
    na, nb = dims
    nd = na * nb
    me_a, me_b = lax.axis_index("tpa"), lax.axis_index("tpb")
    me = me_a * nb + me_b
    npos = h_ref.shape[0]
    ndraft = npos - 1
    nseq = h_ref.shape[1]
    nblk = nseq // LANES
    nunit = nblk * npos
    per_src = nseq // nd
    vloc = w_ref.shape[1]

    def dev(f):
        return {"tpa": f // nb, "tpb": f % nb}

    px, py, pz = me_b % 4, (me_b // 4) % 4, me_b // 16
    xs = [(px + k) % 4 for k in range(4)]
    ys = [((py + k) % 4) * 4 for k in range(4)]
    cores = [me_a, (me_a + 1) % na]

    def each_peer(fn, far=False, own_core=False):
        first = 2 if far else 0

        def plane(kz, carry):
            zz = pz + kz + first
            zz = jnp.where(zz >= 4, zz - 4, zz)
            base = jnp.where(zz >= 4, zz - 4, zz) * 16
            for ky in (2, 1, 3, 0) if far else range(4):
                for kx in (2, 1, 3, 0) if far else (1, 3, 2, 0):
                    for ka in range(1 if own_core else na):
                        b = base + ys[ky] + xs[kx]
                        f = cores[ka] * nb + b
                        ident = {"tpa": cores[ka], "tpb": b}
                        if ka == kx == ky == 0:
                            @pl.when(kz != (4 - first) % 4)
                            def _():
                                fn(f, ident)
                        else:
                            fn(f, ident)
            return carry
        lax.fori_loop(0, 4, plane, 0)

    lane = lax.broadcasted_iota(jnp.int32, (8, LANES), 1)
    sub = lax.broadcasted_iota(jnp.int32, (8, LANES), 0)
    sub4 = lax.broadcasted_iota(jnp.int32, (4, LANES), 0)
    lane_f = lane.astype(F32)
    eye = (lax.broadcasted_iota(jnp.int32, (LANES, LANES), 0) == lax.broadcasted_iota(jnp.int32, (LANES, LANES), 1))

    def to_col(row):
        return jnp.sum(jnp.where(eye, jnp.broadcast_to(row, (LANES, LANES)), 0.0), axis=1, keepdims=True)

    def to_row(col):
        return jnp.sum(jnp.where(eye, jnp.broadcast_to(col, (LANES, LANES)), 0.0), axis=0, keepdims=True)

    def twice(t):
        return jnp.concatenate([t, t], axis=0)

    q_copy = pltpu.make_async_copy(q_ref, qsrc, q_sem)
    q_copy.start()
    w_copy = pltpu.make_async_copy(w_ref, wbuf, w_sem)
    w_copy.start()
    per_pos = nseq // ROWS

    def h_copy(t):
        return pltpu.make_async_copy(h_ref.at[t // per_pos, pl.ds((t % per_pos) * ROWS, ROWS)], hbuf.at[t % NBUF],
                                     h_sem.at[t % NBUF])

    x_copy = pltpu.make_async_copy(xin_ref, x_ref, x_sem)
    x_copy.start()
    for t in range(NBUF - 1):
        h_copy(t).start()

    barrier = pltpu.get_barrier_semaphore()
    each_peer(lambda f, ident: pl.semaphore_signal(barrier, inc=1, device_id=ident, device_id_type=MESH), far=True)
    q_copy.wait()

    def local_bulk(g):
        c0, n = CHUNKS[g]
        return pltpu.make_async_copy(qsrc.at[pl.ds(c0, n), me], qdst.at[me, pl.ds(c0, n)], bulk_rs.at[g])

    for g in range(len(CHUNKS)):
        local_bulk(g).start()
    x_copy.wait()
    xb = x_ref[:, pl.ds(pl.multiple_of((me // 16) * LANES, LANES), LANES)].astype(F32)
    targets = []
    for c in range(per_src):
        j = (me % 16) * per_src + c
        col = jnp.sum(jnp.where(lane[:4] == j, xb, 0.0), axis=1, keepdims=True)
        targets.append(twice(jnp.broadcast_to(col, (4, LANES))) - jnp.where(sub >= 4, F32(LANES), F32(0)) - lane_f)

    def pick_q(d, accs):
        base = (d * vloc).astype(F32)
        return tuple(a + jnp.where(t == base, qsrc[c, d], 0.0) for c, (a, t) in enumerate(zip(accs, targets)))

    accs = lax.fori_loop(0, nd, pick_q, tuple(jnp.zeros((8, LANES), F32) for _ in range(per_src)),
                         unroll=8)
    qp = jnp.zeros((4, LANES), F32)
    for c in range(per_src):
        col = jnp.sum(accs[c], axis=1, keepdims=True)
        qp = jnp.where(lane[:4] == (me % 16) * per_src + c, col[:4] + col[4:], qp)


    def send_bulk(g):
        c0, n = CHUNKS[g]

        def one(c, carry):
            each_peer(lambda f, ident: pltpu.make_async_remote_copy(
                src_ref=qsrc.at[c, f], dst_ref=qdst.at[me, c], send_sem=bulk_ss.at[g], recv_sem=bulk_rs.at[g],
                device_id=ident, device_id_type=MESH).start())
            return carry

        lax.fori_loop(c0, c0 + n, one, 0)

    def wait_bulk(g):
        c0, n = CHUNKS[g]
        ref = qdst.at[:, pl.ds(c0, n)]
        pltpu.make_async_copy(ref, ref, bulk_rs.at[g]).wait()

    w_copy.wait()
    my_base = (me * vloc).astype(F32)
    lane2 = lax.broadcasted_iota(jnp.int32, (LANES, vloc), 1).astype(F32)

    def matmul(t, carry):
        @pl.when(t + NBUF - 1 < npos * per_pos)
        def _():
            h_copy(t + NBUF - 1).start()

        h_copy(t).wait()
        i, r = t // per_pos, t % per_pos
        zb[...] = jnp.dot(hbuf[t % NBUF], wbuf[...], preferred_element_type=F32) * INV_TEMP
        for half in range(ROWS // LANES):
            blk = r * (ROWS // LANES) + half
            zz = zb[half * LANES:(half + 1) * LANES, :]
            m = jnp.max(zz, axis=1, keepdims=True)
            s = jnp.sum(jnp.exp(zz - m), axis=1, keepdims=True)
            ii = jnp.minimum(i, ndraft - 1)
            xblk = x_ref[:, pl.ds(pl.multiple_of(blk * LANES, LANES), LANES)].astype(F32)
            xrow = jnp.sum(jnp.where(sub4 == ii, xblk, 0.0), axis=0, keepdims=True) - my_base
            pick = jnp.sum(jnp.where(lane2 == to_col(xrow), zz, 0.0), axis=1, keepdims=True)
            qrow = jnp.sum(jnp.where((sub4 == ii) & (blk == me // 16), qp, 0.0), axis=0, keepdims=True)
            tile = jnp.where(sub4 == 0, to_row(m), jnp.where(sub4 == 1, to_row(s), jnp.where(
                sub4 == 2, to_row(pick), qrow)))
            st_send[blk * npos + i] = tile

            @pl.when(i < ndraft)
            def _():
                for lt in range(vloc // LANES):
                    zr[pl.ds(blk * LANES * 8 + lt * 4 + i, LANES, stride=8), :] = zz[:, lt * LANES:(lt + 1) * LANES]

            @pl.when(i == ndraft)
            def _():
                z4[pl.ds(pl.multiple_of(blk * LANES, LANES), LANES), :] = zz
        return carry

    lax.fori_loop(0, EARLY, matmul, 0)
    pl.semaphore_wait(barrier, nd - 1)
    send_bulk(0)
    lax.fori_loop(EARLY, npos * per_pos, matmul, 0)

    my_unit = (me_b * 43) % nb
    is_owner = my_unit < nunit

    def send_stats(u, carry):
        chip = (u * 3) % nb
        for a in range(na):
            @pl.when((chip != me_b) | (me_a != a))
            def _():
                pltpu.make_async_remote_copy(src_ref=st_send.at[u], dst_ref=st_recv.at[me], send_sem=st_ss,
                                             recv_sem=st_rs, device_id={"tpa": a, "tpb": chip},
                                             device_id_type=MESH).start()
        return carry

    lax.fori_loop(0, nunit, send_stats, 0)
    send_bulk(1)

    @pl.when(is_owner)
    def _():
        pltpu.make_async_copy(st_send.at[my_unit], st_recv.at[me], st_rs).start()
        pltpu.make_async_copy(st_recv, st_recv, st_rs).wait()
        mx = lax.fori_loop(0, nd, lambda s, m: jnp.maximum(m, st_recv[s]), st_recv[0], unroll=8)[0:1]

        def add(s, carry):
            t = st_recv[s]
            es, zp, qq = carry
            return es + jnp.exp(t[0:1] - mx) * t[1:2], zp + t[2:3], qq + t[3:4]

        zero = jnp.zeros((1, LANES), F32)
        es, zp, qq = lax.fori_loop(0, nd, add, (zero, zero, zero), unroll=8)
        accept = jnp.minimum(1.0, jnp.exp(zp - mx) / es / qq)
        ag_send[...] = jnp.where(sub4 == 0, mx, jnp.where(sub4 == 1, 1.0 / es, accept))
        pltpu.make_async_copy(ag_send, ag_recv.at[my_unit], ag_rs).start()
        each_peer(lambda f, ident: pltpu.make_async_remote_copy(
            src_ref=ag_send, dst_ref=ag_recv.at[my_unit], send_sem=ag_ss, recv_sem=ag_rs, device_id=ident,
            device_id_type=MESH).start(), far=True, own_core=True)

    send_bulk(2)

    pltpu.make_async_copy(ag_recv, ag_recv, ag_rs).wait()
    for g in range(3, len(CHUNKS)):
        send_bulk(g)

    def stat_rows(blk, k):
        return jnp.concatenate([ag_recv[blk * npos + i, k:k + 1, :] for i in range(ndraft)], axis=0)

    def probs(c0, n):
        def body(blk, carry):
            m8, r8 = twice(stat_rows(blk, 0)), twice(stat_rows(blk, 1))
            for j in range(LANES):
                if c0 <= j % per_src < c0 + n:
                    at = pl.ds(pl.multiple_of((blk * LANES + j) * 8, 8), 8)
                    zr[at, :] = jnp.exp(zr[at, :] - m8[:, j:j + 1]) * r8[:, j:j + 1]
            return carry
        lax.fori_loop(0, nblk, body, 0)

    def verdicts(blk, carry):
        a4 = stat_rows(blk, 2)
        cols = pl.ds(pl.multiple_of(blk * LANES, LANES), LANES)
        acc_ref[:, cols] = a4
        run, tot = a4[0:1], a4[0:1]
        for i in range(1, ndraft):
            run = run * a4[i:i + 1]
            tot = tot + run
        exp_ref[:, cols] = tot
        u4 = blk * npos + ndraft
        z4[cols, :] = jnp.exp(z4[cols, :] - to_col(ag_recv[u4, 0:1, :])) * to_col(ag_recv[u4, 1:2, :])
        return carry

    def excess(g):
        c0, n = CHUNKS[g]

        def body(s, accs):
            new = []
            for c in range(n):
                at = pl.ds(pl.multiple_of((s * per_src + c0 + c) * 8, 8), 8)
                e = jnp.maximum(zr[at, :] - qdst[s, c0 + c], 0.0)
                zr[at, :] = e
                new.append(jnp.where(lane == s, jnp.sum(e, axis=1, keepdims=True), accs[c]))
            return tuple(new)

        accs = lax.fori_loop(0, nd, body, tuple(jnp.zeros((8, LANES), F32) for _ in range(n)), unroll=4)
        for c in range(n):
            part = accs[c][:4] + accs[c][4:]
            zs_send[0, (c0 + c) // 2, ((c0 + c) % 2) * 4:((c0 + c) % 2) * 4 + 4] = part

    half = CHUNKS[2][0]
    probs(0, half)
    for g in range(2):
        wait_bulk(g)
        excess(g)
    probs(half, per_src - half)
    for g in range(2, len(CHUNKS)):
        wait_bulk(g)
        excess(g)

    axes = [[{"tpa": cores[a], "tpb": me_b - px + xs[k]} for k in (2, 1, 3, 0) for a in range(na) if (k, a) != (0, 0)],
            [{"tpa": me_a, "tpb": me_b - py * 4 + ys[k]} for k in (2, 1, 3)],
            [{"tpa": me_a, "tpb": me_b - pz * 16 + ((pz + k) % 4) * 16} for k in (2, 1, 3)]]
    first = 0
    for t, group in enumerate(axes):
        for k, ident in enumerate(group):
            pltpu.make_async_remote_copy(src_ref=zs_send.at[t], dst_ref=zs_recv.at[first + k], send_sem=zs_ss.at[t],
                                         recv_sem=zs_rs.at[t], device_id=ident, device_id_type=MESH).start()
        if t == 0:
            lax.fori_loop(0, nblk, verdicts, 0)
        ref = zs_recv.at[pl.ds(first, len(group))]
        pltpu.make_async_copy(ref, ref, zs_rs.at[t]).wait()
        total = zs_send[t]
        for k in range(len(group)):
            total = total + zs_recv[first + k]
        if t + 1 < len(axes):
            zs_send[t + 1] = total
        else:
            rz_ref[...] = 1.0 / total
        first += len(group)

    def drain(ref, sem):
        pltpu.make_async_copy(ref, ref, sem).wait()

    for g, (c0, n) in enumerate(CHUNKS):
        drain(qsrc.at[pl.ds(c0, n), pl.ds(0, nd - 1)], bulk_ss.at[g])

    @pl.when(is_owner)
    def _():
        drain(st_send, st_ss)
        drain(st_send.at[pl.ds(0, nunit - 1)], st_ss)
        drain(st_recv.at[pl.ds(0, nb - 1)], ag_ss)

    @pl.when(jnp.logical_not(is_owner))
    def _():
        drain(st_send, st_ss)
        drain(st_send, st_ss)

    for t, group in enumerate(axes):
        drain(zs_recv.at[pl.ds(0, len(group))], zs_ss.at[t])


def write_out(acc_ref, exp_ref, num_ref, bon_ref, rz_ref, acc_out, exp_out, res_out, bon_out, res, sem):
    nd, per_src = num_ref.shape[:2]
    small = [pltpu.make_async_copy(a, b, sem.at[k]) for k, (a, b) in enumerate(
        ((acc_ref, acc_out), (exp_ref, exp_out), (bon_ref, bon_out)))]
    for c in small:
        c.start()

    def put(c):
        return pltpu.make_async_copy(res.at[:, c], res_out.at[:, c], sem.at[3 + c])

    for c in range(per_src):
        tile = rz_ref[c // 2, (c % 2) * 4:(c % 2) * 4 + 4]
        r8 = jnp.concatenate([tile, tile], axis=0)
        for s in range(nd):
            res[s, c] = num_ref[s, c] * r8[:, s:s + 1]
        put(c).start()
    for c in range(per_src):
        put(c).wait()
    for c in small:
        c.wait()


def solution(mesh):
    na, nb = mesh.shape["tpa"], mesh.shape["tpb"]
    nd = na * nb

    def local_step(hidden, w_head, q_draft, x_draft):
        nseq, npos, dm = hidden.shape
        ndraft = npos - 1
        vloc = w_head.shape[1]
        per_src = q_draft.shape[0]
        nt = vloc // LANES
        h5 = jnp.transpose(hidden, (1, 0, 2))
        q4 = q_draft.reshape(per_src, ndraft, nd, nt, LANES).transpose(0, 2, 3, 1, 4).reshape(per_src, nd, nt * ndraft,
                                                                                             LANES)
        xt = x_draft.T
        nunit = (nseq // LANES) * npos
        hbm = pl.BlockSpec(memory_space=pltpu.HBM)
        vmem = pl.BlockSpec(memory_space=pltpu.VMEM)
        dma, vm = pltpu.SemaphoreType.DMA, pltpu.VMEM
        outs = pl.pallas_call(
            functools.partial(kernel, (na, nb)),
            out_shape=[
                jax.ShapeDtypeStruct((ndraft, nseq), F32),
                jax.ShapeDtypeStruct((1, nseq), F32),
                jax.ShapeDtypeStruct((nseq * nt * ndraft, LANES), F32),
                jax.ShapeDtypeStruct((nseq, vloc), F32),
                jax.ShapeDtypeStruct((per_src // 2, 8, LANES), F32),
            ],
            in_specs=[hbm] * 4,
            out_specs=[vmem] * 5,
            scratch_shapes=[
                vm((NBUF, ROWS, dm), jnp.bfloat16),
                vm((dm, vloc), jnp.bfloat16),
                vm((ndraft, nseq), jnp.int32),
                vm((per_src, nd, 8, LANES), F32),
                vm((nd, per_src, 8, LANES), F32),
                vm((ROWS, vloc), F32),
                vm((nunit, 4, LANES), F32),
                vm((nd, 4, LANES), F32),
                vm((4, LANES), F32),
                vm((nunit, 4, LANES), F32),
                vm((3, per_src // 2, 8, LANES), F32),
                vm((13, per_src // 2, 8, LANES), F32),
                dma((NBUF,)), dma, dma, dma, dma((len(CHUNKS),)), dma((len(CHUNKS),)), dma, dma, dma, dma, dma((3,)),
                dma((3,)),
            ],
            compiler_params=pltpu.CompilerParams(collective_id=0, has_side_effects=True,
                                                 vmem_limit_bytes=46 * 1024 * 1024),
            name="verify",
        )(*[pltpu.with_memory_space_constraint(a, pltpu.HBM) for a in (h5, w_head, q4, xt)])
        acc, exp, num, bonus, rz = outs
        num = num.reshape(nd, per_src, nt * ndraft, LANES)
        outs = (acc, exp, num, bonus)
        acc, exp, res, bonus = pl.pallas_call(
            write_out,
            out_shape=[jax.ShapeDtypeStruct(o.shape, o.dtype) for o in outs],
            in_specs=[vmem] * 5,
            out_specs=[hbm] * 4,
            scratch_shapes=[vm(num.shape, F32), dma((3 + per_src,))],
            compiler_params=pltpu.CompilerParams(vmem_limit_bytes=8 * 1024 * 1024),
            name="write_out",
        )(*outs, rz)
        residual = res.reshape(nseq, nt, ndraft, LANES).transpose(0, 2, 1, 3).reshape(nseq, ndraft, vloc)
        return acc.T, exp.reshape(nseq), residual, bonus

    return jax.shard_map(
        local_step, mesh=mesh,
        in_specs=(P("dp", None, None), P(None, VOCAB_AXES), P(("dp",) + VOCAB_AXES, None, None), P("dp", None)),
        out_specs=(P("dp", None), P("dp"), P("dp", None, VOCAB_AXES), P("dp", VOCAB_AXES)),
        check_vma=False)
```
